32 devices in a mesh: rep: 1 (over z), wg: 32 (over y, x, core).
Axes of the slice: x: 4, y: 4, z: 1, core: 2. Of those that a mesh axis runs over, the one named last changes fastest.
The devices are a block of a 4x4x8 slice.
Arguments:
- x_in: bfloat16 [32, 1024, 3072], P(('rep', 'wg'))
- lengths: int32 [32], P(('rep', 'wg'))
- positions: int32 [32, 1024], P(('rep', 'wg'))
- w_q: bfloat16 [3072, 3072], P('wg')
- w_k: bfloat16 [3072, 1024], P('wg')
- w_v: bfloat16 [3072, 1024], P('wg')
- w_o: bfloat16 [3072, 3072], P('wg')
- w_up: bfloat16 [3072, 9216], P('wg')
- w_down: bfloat16 [9216, 3072], P('wg')
- ln1_gain: float32 [3072], P('wg')
- ln1_bias: float32 [3072], P('wg')
- ln2_gain: float32 [3072], P('wg')
- ln2_bias: float32 [3072], P('wg')
Outputs:
- output 1: bfloat16 [32, 1024, 3072], P(('rep', 'wg'))
- output 2: bfloat16 [32, 1024, 8, 128], P(('rep', 'wg'))
- output 3: bfloat16 [32, 1024, 8, 128], P(('rep', 'wg'))
All inputs are finite; a program needn't handle non-finite values.
Results may differ from the reference program's by a relative error of at most 0.0096177.
Values are sent between devices in bfloat16 or wider.
A program may use at most 768 MiB of HBM per device.

```python
import jax
import jax.numpy as jnp
from jax import lax

BATCH_PART = 32
SEQ_LEN = 1024
D_MODEL = 3072
HEADS = 24
KV_HEADS = 8
HEAD_DIM = 128
FF_DIM = 9216
Q_BLOCK = min(SEQ_LEN, 128)
LN_EPS = 1e-5
ROPE_BASE = 10000.0


def draw_lengths(len_key):
    base_len = jax.random.randint(len_key, (BATCH_PART,), 1, SEQ_LEN + 1)
    full_slot = jax.random.randint(jax.random.fold_in(len_key, 1), (), 0, BATCH_PART)
    return jnp.where(jnp.arange(BATCH_PART) == full_slot, SEQ_LEN, base_len).astype(jnp.int32)


def draw_positions(pos_key):
    start_key, step_key = jax.random.split(pos_key)
    starts = jax.random.randint(start_key, (BATCH_PART, 1), 0, SEQ_LEN)
    pos_steps = jax.random.randint(step_key, (BATCH_PART, SEQ_LEN), 1, 4)
    return (starts + jnp.cumsum(pos_steps, axis=1) - pos_steps[:, :1]).astype(jnp.int32)


def normal_weight(w_key, n_rows, n_cols, scale_mult):
    values = jax.random.normal(w_key, (n_rows, n_cols), jnp.float32)
    return (values * (scale_mult * n_rows ** -0.5)).astype(jnp.bfloat16)


def setup_inputs(seed: int = 0, part: int = 0) -> dict:
    part_key = jax.random.fold_in(jax.random.key(seed), part)
    act_key, len_key, pos_key = jax.random.split(part_key, 3)
    weight_keys = jax.random.split(jax.random.key(seed + 1), 10)
    x_in = jax.random.normal(act_key, (BATCH_PART, SEQ_LEN, D_MODEL), jnp.float32).astype(jnp.bfloat16)
    return {
        "x_in": x_in,
        "lengths": draw_lengths(len_key),
        "positions": draw_positions(pos_key),
        "w_q": normal_weight(weight_keys[0], D_MODEL, HEADS * HEAD_DIM, 2.0),
        "w_k": normal_weight(weight_keys[1], D_MODEL, KV_HEADS * HEAD_DIM, 2.0),
        "w_v": normal_weight(weight_keys[2], D_MODEL, KV_HEADS * HEAD_DIM, 1.0),
        "w_o": normal_weight(weight_keys[3], HEADS * HEAD_DIM, D_MODEL, 1.0),
        "w_up": normal_weight(weight_keys[4], D_MODEL, FF_DIM, 1.0),
        "w_down": normal_weight(weight_keys[5], FF_DIM, D_MODEL, 1.0),
        "ln1_gain": 0.3 * jax.random.normal(weight_keys[6], (D_MODEL,), jnp.float32),
        "ln1_bias": 0.3 * jax.random.normal(weight_keys[7], (D_MODEL,), jnp.float32),
        "ln2_gain": 0.3 * jax.random.normal(weight_keys[8], (D_MODEL,), jnp.float32),
        "ln2_bias": 0.3 * jax.random.normal(weight_keys[9], (D_MODEL,), jnp.float32),
    }


def layer_norm1p(acts, ln_gain, ln_bias):
    acts_f = acts.astype(jnp.float32)
    row_mean = jnp.mean(acts_f, axis=-1, keepdims=True)
    centered = acts_f - row_mean
    variance = jnp.mean(centered * centered, axis=-1, keepdims=True)
    return (centered * lax.rsqrt(variance + LN_EPS) * (1.0 + ln_gain) + ln_bias).astype(jnp.bfloat16)


def apply_rotary(proj, cos_tab, sin_tab):
    quarter = proj.shape[-1] // 4
    rot_lo = proj[..., :quarter]
    rot_hi = proj[..., quarter:2 * quarter]
    return jnp.concatenate([rot_lo * cos_tab - rot_hi * sin_tab, rot_hi * cos_tab + rot_lo * sin_tab, proj[..., 2 * quarter:]], axis=-1)


def reference(x_in, lengths, positions, w_q, w_k, w_v, w_o, w_up, w_down, ln1_gain, ln1_bias, ln2_gain, ln2_bias):
    group_size = HEADS // KV_HEADS
    quarter = HEAD_DIM // 4
    inv_freq = ROPE_BASE ** (-jnp.arange(quarter, dtype=jnp.float32) / quarter)
    key_idx = jnp.arange(SEQ_LEN)
    score_scale = HEAD_DIM ** -0.5

    def one_sequence(seq_args):
        x_seq, seq_length, pos_seq = seq_args
        angles = pos_seq.astype(jnp.float32)[:, None, None] * inv_freq
        cos_tab = jnp.cos(angles)
        sin_tab = jnp.sin(angles)
        h_norm = layer_norm1p(x_seq, ln1_gain, ln1_bias)
        q_acc = jnp.dot(h_norm, w_q, preferred_element_type=jnp.float32).reshape(SEQ_LEN, HEADS, HEAD_DIM)
        k_acc = jnp.dot(h_norm, w_k, preferred_element_type=jnp.float32).reshape(SEQ_LEN, KV_HEADS, HEAD_DIM)
        v_acc = jnp.dot(h_norm, w_v, preferred_element_type=jnp.float32).reshape(SEQ_LEN, KV_HEADS, HEAD_DIM)
        tok_valid = (key_idx < seq_length)[:, None, None]
        q_rot = apply_rotary(q_acc, cos_tab, sin_tab).astype(jnp.bfloat16)
        k_keep = jnp.where(tok_valid, apply_rotary(k_acc, cos_tab, sin_tab).astype(jnp.bfloat16), 0)
        v_keep = jnp.where(tok_valid, v_acc.astype(jnp.bfloat16), 0)
        q_blocks = q_rot.reshape(SEQ_LEN // Q_BLOCK, Q_BLOCK, KV_HEADS, group_size, HEAD_DIM)
        k_f32 = k_keep.astype(jnp.float32)
        v_f32 = v_keep.astype(jnp.float32)

        def one_block(blk_args):
            q_blk, blk_start = blk_args
            scores = jnp.einsum("qkgd,skd->kgqs", q_blk.astype(jnp.float32), k_f32) * score_scale
            query_idx = blk_start + jnp.arange(Q_BLOCK)
            allowed = (key_idx[None, :] <= query_idx[:, None]) & (key_idx[None, :] < seq_length)
            scores = jnp.where(allowed, scores, -1e30)
            prob_bf = jax.nn.softmax(scores, axis=-1).astype(jnp.bfloat16)
            att_blk = jnp.einsum("kgqs,skd->qkgd", prob_bf.astype(jnp.float32), v_f32)
            return att_blk.astype(jnp.bfloat16)

        att_all = lax.map(one_block, (q_blocks, jnp.arange(SEQ_LEN // Q_BLOCK) * Q_BLOCK))
        att_flat = att_all.reshape(SEQ_LEN, HEADS * HEAD_DIM)
        o_acc = jnp.dot(att_flat, w_o, preferred_element_type=jnp.float32)
        x_mid = (x_seq.astype(jnp.float32) + o_acc).astype(jnp.bfloat16)
        h_mid = layer_norm1p(x_mid, ln2_gain, ln2_bias)
        up_acc = jnp.dot(h_mid, w_up, preferred_element_type=jnp.float32)
        sq_relu = jnp.square(jnp.maximum(up_acc, 0.0)).astype(jnp.bfloat16)
        down_acc = jnp.dot(sq_relu, w_down, preferred_element_type=jnp.float32)
        y_seq = (x_mid.astype(jnp.float32) + down_acc).astype(jnp.bfloat16)
        return y_seq, k_keep, v_keep

    y_out, k_cache, v_cache = lax.map(one_sequence, (x_in, lengths, positions))
    return y_out, k_cache, v_cache
```

```python
import functools
import math

import jax
import jax.numpy as jnp
from jax import lax
from jax.experimental import pallas as pl
from jax.experimental.pallas import tpu as pltpu
from jax.sharding import PartitionSpec as P

LN_EPS = 1e-5
ROPE_BASE = 10000.0
HEAD_DIM = 128
LANES = 128
MESH = pl.DeviceIdType.MESH
F32 = jnp.float32
BF16 = jnp.bfloat16


def rotary_tables(positions):
    quarter = HEAD_DIM // 4
    inv_freq = ROPE_BASE ** (-jnp.arange(quarter, dtype=F32) / quarter)
    angles = positions.astype(F32)[:, None] * inv_freq
    cos, sin = jnp.cos(angles), jnp.sin(angles)
    pad = jnp.zeros((positions.shape[0], 2 * quarter), F32)
    return jnp.concatenate([cos, cos, pad], axis=1), jnp.concatenate([-sin, sin, pad], axis=1)


def layer_kernel(cfg, len_ref, cos_ref, sin_ref, x_ref, ln_ref, wq_ref, wk_ref, wv_ref, wo_ref, wu_ref, wd_ref,
                 y_ref, k_out, v_out, gln, gq, gk, gv, go, gu, gd,
                 x_s, h_s, q_s, k_s, v_s, a_s, wb, wbd, acc_s, lnv, lnbuf, lnst,
                 send_sem, recv_sem, stage_sem, own_sem, wb_sem, wbd_sem, io_sem):
    side = cfg["side"]
    seq, d_model = x_s.shape
    n_heads, n_kv = q_s.shape[0], k_s.shape[0]
    tile, rows_m = cfg["tile"], cfg["rows_m"]
    me = lax.axis_index("wg")
    c = lax.rem(me, 2)
    x = lax.rem(me // 2, side)
    y = me // (2 * side)
    xp, xm = lax.rem(x + 1, side), lax.rem(x + side - 1, side)
    yp, ym = lax.rem(y + 1, side), lax.rem(y + side - 1, side)
    xo, yo = lax.rem(x + 2, side), lax.rem(y + 2, side)

    def device(yy, xx, cc):
        return (yy * side + xx) * 2 + cc

    d_xp, d_xm, d_yp, d_ym = device(y, xp, c), device(y, xm, c), device(yp, x, c), device(ym, x, c)
    d_peer = device(y, x, 1 - c)

    barrier = pltpu.get_barrier_semaphore()
    for dev in (d_xp, d_xm, d_yp, d_ym, d_peer):
        pl.semaphore_signal(barrier, inc=1, device_id={"wg": dev}, device_id_type=MESH)
    pl.semaphore_wait(barrier, 5)

    shards = {"ln": (ln_ref, gln), "q": (wq_ref, gq), "k": (wk_ref, gk), "v": (wv_ref, gv), "o": (wo_ref, go),
              "u": (wu_ref, gu), "d": (wd_ref, gd)}
    blocks = cfg["blocks"]

    def put(blk, phase, src, dst, dev):
        pltpu.make_async_remote_copy(
            src_ref=src, dst_ref=dst, send_sem=send_sem.at[blk, phase], recv_sem=recv_sem.at[blk, phase],
            device_id={"wg": dev}, device_id_type=MESH).start()

    def same(blk, phase, ref, dev):
        put(blk, phase, ref, ref, dev)

    def cols_of(blk):
        name, c0, width = blocks[blk]
        half, quarter = width // 2, width // 4
        return (pl.ds(c0, half), pl.ds(c0, quarter), pl.ds(c0 + quarter, quarter),
                pl.ds(c0 + half, half), pl.ds(c0 + half, quarter), pl.ds(c0 + half + quarter, quarter), pl.ds(c0, width))

    def unit_refs(blk):
        name, c0, width = blocks[blk]
        g = shards[name][1]
        cw = pl.ds(c0, width)
        return (g.at[0, pl.ds(0, 2), 0, :, cw], g.at[0, 0, 0, :, cw], g.at[0, :, :, :, cw],
                g.at[0, :, 0, :, cw], g.at[:, :, 0, :, cw])

    def wait_on(ref, sem):
        pltpu.make_async_copy(ref, ref, sem).wait()

    def wait_recv(blk, phase):
        wait_on(unit_refs(blk)[phase], recv_sem.at[blk, phase])

    def wait_send(blk):
        for phase, ref in enumerate(unit_refs(blk)):
            wait_on(ref, send_sem.at[blk, phase])

    def phase_1a(blk):
        w, g = shards[blocks[blk][0]]
        ca, _, _, cb, _, _, cw = cols_of(blk)
        put(blk, 0, w.at[:, ca], g.at[y, x, c, :, ca], d_xp)
        put(blk, 0, w.at[:, ca], g.at[y, x, c, :, ca], d_xm)
        put(blk, 0, w.at[:, cb], g.at[y, x, c, :, cb], d_yp)
        put(blk, 0, w.at[:, cb], g.at[y, x, c, :, cb], d_ym)
        put(blk, 4, w.at[:, cw], g.at[y, x, c, :, cw], d_peer)

    def phase_1b(blk):
        g = shards[blocks[blk][0]][1]
        ca, a0, a1, cb, b0, b1, _ = cols_of(blk)
        wait_recv(blk, 0)
        same(blk, 1, g.at[y, xm, c, :, a0], d_xp)
        same(blk, 1, g.at[y, xp, c, :, a1], d_xm)
        same(blk, 1, g.at[ym, x, c, :, b0], d_yp)
        same(blk, 1, g.at[yp, x, c, :, b1], d_ym)
        same(blk, 4, g.at[y, xm, c, :, ca], d_peer)
        same(blk, 4, g.at[y, xp, c, :, ca], d_peer)
        same(blk, 4, g.at[ym, x, c, :, cb], d_peer)
        same(blk, 4, g.at[yp, x, c, :, cb], d_peer)

    def phase_2a(blk):
        g = shards[blocks[blk][0]][1]
        ca, _, _, cb, _, _, _ = cols_of(blk)
        wait_recv(blk, 1)
        same(blk, 2, g.at[y, :, c, :, ca], d_yp)
        same(blk, 2, g.at[y, :, c, :, ca], d_ym)
        same(blk, 2, g.at[:, x, c, :, cb], d_xp)
        same(blk, 2, g.at[:, x, c, :, cb], d_xm)
        same(blk, 4, g.at[y, xo, c, :, ca], d_peer)
        same(blk, 4, g.at[yo, x, c, :, cb], d_peer)

    def phase_2b(blk):
        g = shards[blocks[blk][0]][1]
        ca, a0, a1, cb, b0, b1, _ = cols_of(blk)
        same(blk, 3, g.at[ym, :, c, :, a0], d_yp)
        same(blk, 3, g.at[yp, :, c, :, a1], d_ym)
        same(blk, 3, g.at[:, xm, c, :, b0], d_xp)
        same(blk, 3, g.at[:, xp, c, :, b1], d_xm)
        same(blk, 4, g.at[ym, :, c, :, ca], d_peer)
        same(blk, 4, g.at[yp, :, c, :, ca], d_peer)
        same(blk, 4, g.at[:, xm, c, :, cb], d_peer)
        same(blk, 4, g.at[:, xp, c, :, cb], d_peer)

    def finish(blk):
        g = shards[blocks[blk][0]][1]
        ca, _, _, cb, _, _, _ = cols_of(blk)
        wait_recv(blk, 3)
        same(blk, 4, g.at[yo, :, c, :, ca], d_peer)
        same(blk, 4, g.at[:, xo, c, :, cb], d_peer)

    def ready(blk):
        wait_recv(blk, 4)

    n_blk = len(blocks)

    def service(j):
        wait_recv(j, 2)
        if j + 1 < n_blk:
            phase_2a(j + 1)
        phase_2b(j)
        if j + 3 < n_blk:
            phase_1b(j + 3)
        if j + 5 < n_blk:
            phase_1a(j + 5)

    def matmul_tiles(g, col0, n_tiles, epilogue):
        def fetch(t, slot):
            return pltpu.make_async_copy(
                g.at[:, :, :, :, pl.ds(pl.multiple_of(col0 + t * tile, LANES), tile)], wb.at[slot], wb_sem.at[slot])

        fetch(0, 0).start()

        @pl.loop(0, n_tiles)
        def _(t):
            slot = lax.rem(t, 2)

            @pl.when(t + 1 < n_tiles)
            def _():
                fetch(t + 1, lax.rem(t + 1, 2)).start()

            fetch(t, slot).wait()

            @pl.loop(0, seq // rows_m)
            def _(m):
                rows = pl.ds(pl.multiple_of(m * rows_m, rows_m), rows_m)
                weights = wb[slot].reshape(d_model, tile)
                epilogue(t, rows, m, jnp.dot(h_s[rows, :], weights, preferred_element_type=F32))

    lane = lax.broadcasted_iota(jnp.int32, (rows_m, HEAD_DIM), 1)
    eighth = HEAD_DIM // 4

    def rotate(vals, rows):
        swapped = jnp.where(lane < eighth, pltpu.roll(vals, HEAD_DIM - eighth, 1), pltpu.roll(vals, eighth, 1))
        turned = vals * cos_ref[rows, :] + swapped * sin_ref[rows, :]
        return jnp.where(lane < 2 * eighth, turned, vals)

    heads_per_tile = tile // HEAD_DIM
    length = len_ref[0]

    def q_tiles(col0, width):
        def epilogue(t, rows, m, acc):
            for i in range(heads_per_tile):
                part = acc[:, i * HEAD_DIM:(i + 1) * HEAD_DIM]
                q_s[col0 // HEAD_DIM + t * heads_per_tile + i, rows, :] = rotate(part, rows).astype(BF16)

        matmul_tiles(gq, col0, width // tile, epilogue)

    def kv_tiles(g, out, turn, width):
        def epilogue(t, rows, m, acc):
            token = m * rows_m + lax.broadcasted_iota(jnp.int32, (rows_m, HEAD_DIM), 0)
            for i in range(heads_per_tile):
                part = acc[:, i * HEAD_DIM:(i + 1) * HEAD_DIM]
                part = rotate(part, rows) if turn else part
                kept = jnp.where(token < length, part, 0.0).astype(BF16)
                out[t * heads_per_tile + i, rows, :] = kept

        matmul_tiles(g, 0, width // tile, epilogue)

    per_kv = n_heads // n_kv
    q_rows = cfg["q_rows"]
    score_scale = HEAD_DIM ** -0.5

    def attention(g_lo, g_hi):
        @pl.loop(g_lo, g_hi)
        def _(kv):
            for blk in range(seq // q_rows):
                lo, hi = blk * q_rows, (blk + 1) * q_rows
                key = lax.broadcasted_iota(jnp.int32, (q_rows, hi), 1)
                query = lo + lax.broadcasted_iota(jnp.int32, (q_rows, hi), 0)
                allowed = (key <= query) & (key < length)
                for i in range(per_kv):
                    head = kv * per_kv + i
                    scores = lax.dot_general(q_s[head, lo:hi, :], k_s[kv, :hi, :], (((1,), (1,)), ((), ())),
                                             preferred_element_type=F32) * score_scale
                    scores = jnp.where(allowed, scores, -1e30)
                    probs = jnp.exp(scores - jnp.max(scores, axis=1, keepdims=True))
                    probs = probs * (1.0 / jnp.sum(probs, axis=1, keepdims=True))
                    out = jnp.dot(probs.astype(BF16), v_s[kv, :hi, :], preferred_element_type=F32)
                    h_s[lo:hi, pl.ds(pl.multiple_of(head * HEAD_DIM, HEAD_DIM), HEAD_DIM)] = out.astype(BF16)

    def o_tiles(col0, width):
        def epilogue(t, rows, m, acc):
            cols = pl.ds(pl.multiple_of(col0 + t * tile, LANES), tile)
            x_s[rows, cols] = (x_s[rows, cols].astype(F32) + acc).astype(BF16)

        matmul_tiles(go, col0, width // tile, epilogue)

    def up_tiles(col0, width):
        def epilogue(t, rows, m, acc):
            cols = pl.ds(pl.multiple_of(col0 + t * tile, LANES), tile)
            a_s[rows, cols] = jnp.square(jnp.maximum(acc, 0.0)).astype(BF16)

        matmul_tiles(gu, col0, width // tile, epilogue)

    def down_tile(col0):
        cols = pl.ds(col0, tile)
        depth = a_s.shape[1] // side

        def fetch(k, slot):
            return pltpu.make_async_copy(gd.at[k, :, :, :, cols], wbd.at[slot], wbd_sem.at[slot])

        fetch(0, 0).start()

        @pl.loop(0, side)
        def _(k):
            slot = lax.rem(k, 2)

            @pl.when(k + 1 < side)
            def _():
                fetch(k + 1, lax.rem(k + 1, 2)).start()

            fetch(k, slot).wait()
            deep = pl.ds(pl.multiple_of(k * depth, LANES), depth)

            @pl.loop(0, seq // rows_m)
            def _(m):
                rows = pl.ds(pl.multiple_of(m * rows_m, rows_m), rows_m)
                part = jnp.dot(a_s[rows, deep], wbd[slot].reshape(depth, tile), preferred_element_type=F32)
                acc_s[rows, :] = jnp.where(k == 0, part, acc_s[rows, :] + part)

        @pl.loop(0, seq // rows_m)
        def _(m):
            rows = pl.ds(pl.multiple_of(m * rows_m, rows_m), rows_m)
            x_s[rows, cols] = (x_s[rows, cols].astype(F32) + acc_s[rows, :]).astype(BF16)

        pltpu.make_async_copy(x_s.at[:, cols], y_ref.at[:, cols], io_sem.at[3]).start()

    def gather_norms():
        pltpu.make_async_copy(gln.at[:, :, :, :, pl.ds(0, 2 * LANES)], lnbuf, io_sem.at[4]).start()
        wait_on(lnbuf, io_sem.at[4])
        lnv[...] = jnp.zeros_like(lnv)
        share = cfg["share"]
        for dev in range(2 * side * side):
            start = dev * share // LANES * LANES
            width = min(2 * LANES, d_model - start)
            lnv[:, start:start + width] += lnbuf[dev // (2 * side), dev // 2 % side, dev % 2, :, :width]

    ln_rows = cfg["ln_rows"]

    def normalize(which):
        @pl.loop(0, seq // ln_rows)
        def _(m):
            rows = pl.ds(pl.multiple_of(m * ln_rows, ln_rows), ln_rows)
            acts = x_s[rows, :].astype(F32)
            centered = acts - jnp.mean(acts, axis=1, keepdims=True)
            variance = jnp.mean(centered * centered, axis=1, keepdims=True)
            gain, bias = lnv[which:which + 1, :], lnv[which + 1:which + 2, :]
            h_s[rows, :] = (centered * lax.rsqrt(variance + LN_EPS) * (1.0 + gain) + bias).astype(BF16)

    for blk in range(3):
        phase_1a(blk)
    pltpu.make_async_copy(x_ref, x_s, io_sem.at[0]).start()
    staged = []
    for idx, (name, r0, c0) in enumerate(cfg["staging"]):
        src = shards[name][0]
        spot = a_s.at[pl.ds(r0, src.shape[0]), pl.ds(c0, src.shape[1])]
        staged.append((shards[name][1], spot, src))
        pltpu.make_async_copy(src, spot, stage_sem.at[idx]).start()
    staged.append((gln, lnst, ln_ref))
    pltpu.make_async_copy(ln_ref, lnst, stage_sem.at[len(staged) - 1]).start()
    for idx, (g, spot, src) in enumerate(staged):
        wait_on(spot, stage_sem.at[idx])
        pltpu.make_async_copy(spot, g.at[y, x, c], own_sem.at[idx]).start()
    phase_1b(0)
    phase_1a(3)
    for idx, (g, spot, src) in enumerate(staged):
        wait_on(spot, own_sem.at[idx])
    phase_2a(0)
    phase_1b(1)
    phase_1a(4)
    phase_1b(2)

    kv_width, q_half, up_part = gk.shape[-1], gq.shape[-1] // 2, gu.shape[-1] // 6

    def first_norm():
        wait_on(x_s, io_sem.at[0])
        gather_norms()
        normalize(0)

    def k_part():
        kv_tiles(gk, k_s, True, kv_width)
        pltpu.make_async_copy(k_s, k_out, io_sem.at[1]).start()

    def v_part():
        kv_tiles(gv, v_s, False, kv_width)
        pltpu.make_async_copy(v_s, v_out, io_sem.at[2]).start()

    def up(i):
        return lambda: up_tiles(i * up_part, up_part)

    def down(i):
        return lambda: down_tile(i * tile)

    def blocks_in(*ids):
        def take():
            for blk in ids:
                ready(blk)
        return take

    half_kv = n_kv // 2
    plan = {
        2: ((blocks_in(0), first_norm), ()),
        3: ((blocks_in(1), k_part), ()),
        4: ((blocks_in(2), v_part), ()),
        5: ((blocks_in(3), lambda: q_tiles(0, q_half)), ()),
        6: ((blocks_in(4), lambda: q_tiles(q_half, q_half)), ()),
        7: ((lambda: attention(0, half_kv // 2),), (lambda: attention(half_kv // 2, half_kv),)),
        8: ((lambda: attention(half_kv, half_kv + half_kv // 2),), (lambda: attention(half_kv + half_kv // 2, n_kv),)),
        9: ((blocks_in(5, 6), lambda: o_tiles(0, q_half)), (lambda: o_tiles(q_half, q_half),)),
        10: ((lambda: normalize(2),), (blocks_in(7), up(0))),
        11: ((blocks_in(8), up(1)), (blocks_in(9), up(2))),
        12: ((blocks_in(10), up(3)), ()),
        13: ((blocks_in(11), up(4)), ()),
        14: ((blocks_in(12), up(5)), ()),
        15: ((blocks_in(13), down(0)), ()),
        16: ((blocks_in(14), down(1)), ()),
        17: ((blocks_in(15), down(2)), ()),
        18: ((blocks_in(16), down(3)), ()),
    }
    for j in range(n_blk):
        service(j)
        early, late = plan.get(j, ((), ()))
        for piece in early:
            piece()
        if j >= 1:
            finish(j - 1)
        for piece in late:
            piece()
    finish(n_blk - 1)
    ready(17)
    down_tile(4 * tile)
    ready(18)
    down_tile(5 * tile)
    wait_on(k_s, io_sem.at[1])
    wait_on(v_s, io_sem.at[2])
    wait_on(x_s, io_sem.at[3])
    for blk in range(n_blk):
        wait_send(blk)


def run_layer(n, x_loc, len_loc, cos_tab, sin_tab, ln_part, wq, wk, wv, wo, wu, wd, scale=1):
    seq, d_model = x_loc.shape
    side = math.isqrt(n // 2)
    tile = 512 // scale
    nq, nkv, ff = wq.shape[1], wk.shape[1], wu.shape[1]
    half = nq // 2
    blocks = [("ln", 0, ln_part.shape[1]), ("k", 0, nkv), ("v", 0, nkv), ("q", 0, half), ("q", half, half),
              ("o", 0, d_model // 2), ("o", d_model // 2, d_model // 2)]
    blocks += [("u", i * (ff // 6), ff // 6) for i in range(6)]
    blocks += [("d", i * (d_model // 6), d_model // 6) for i in range(6)]
    share = wq.shape[0]
    staging = [("q", 0, 0), ("k", 0, nq), ("v", 0, nq + nkv), ("o", 0, nq + 2 * nkv), ("u", share, 0), ("d", 2 * share, 0)]
    cfg = dict(side=side, tile=tile, rows_m=512 // scale, q_rows=256 // scale, ln_rows=64, share=share, blocks=blocks,
               staging=staging)
    vmem, hbm = pltpu.VMEM, pl.BlockSpec(memory_space=pltpu.HBM)

    def gathered(part):
        return jax.ShapeDtypeStruct((side, side, 2) + part.shape, part.dtype)

    flops = 2 * seq * (d_model * (nq + 2 * nkv + ff) + nq * d_model + ff * d_model)
    outs = pl.pallas_call(
        functools.partial(layer_kernel, cfg),
        out_shape=[jax.ShapeDtypeStruct((seq, d_model), BF16), jax.ShapeDtypeStruct((nkv // HEAD_DIM, seq, HEAD_DIM), BF16),
                   jax.ShapeDtypeStruct((nkv // HEAD_DIM, seq, HEAD_DIM), BF16)]
        + [gathered(part) for part in (ln_part, wq, wk, wv, wo, wu, wd)],
        in_specs=[pl.BlockSpec(memory_space=pltpu.SMEM), pl.BlockSpec(memory_space=vmem), pl.BlockSpec(memory_space=vmem)] + [hbm] * 8,
        out_specs=[hbm] * 10,
        scratch_shapes=[
            vmem((seq, d_model), BF16), vmem((seq, d_model), BF16), vmem((nq // HEAD_DIM, seq, HEAD_DIM), BF16),
            vmem((nkv // HEAD_DIM, seq, HEAD_DIM), BF16), vmem((nkv // HEAD_DIM, seq, HEAD_DIM), BF16), vmem((seq, ff), BF16),
            vmem((2, side, side, 2, share, tile), BF16), vmem((2, side, 2, wd.shape[0], tile), BF16), vmem((seq, tile), F32),
            vmem((ln_part.shape[0], d_model), F32), vmem((side, side, 2, ln_part.shape[0], 2 * LANES), F32), vmem(ln_part.shape, F32),
            pltpu.SemaphoreType.DMA((len(blocks), 5)), pltpu.SemaphoreType.DMA((len(blocks), 5)),
            pltpu.SemaphoreType.DMA((7,)), pltpu.SemaphoreType.DMA((7,)), pltpu.SemaphoreType.DMA((2,)),
            pltpu.SemaphoreType.DMA((2,)), pltpu.SemaphoreType.DMA((5,)),
        ],
        compiler_params=pltpu.CompilerParams(collective_id=0, has_side_effects=True, vmem_limit_bytes=67043328),
        cost_estimate=pl.CostEstimate(flops=flops, bytes_accessed=4 * n * wd.size, transcendentals=0),
    )(len_loc, cos_tab, sin_tab, x_loc, ln_part, wq, wk, wv, wo, wu, wd)
    return outs[:3]


def solution(mesh, scale=1):
    batch_spec = P(("rep", "wg"))
    row_spec = P("wg")
    n = mesh.shape["wg"]

    def local_layer(x_loc, lengths, positions, wq, wk, wv, wo, wu, wd, gain1, bias1, gain2, bias2):
        n_seq, seq, d_model = x_loc.shape
        cos_tab, sin_tab = rotary_tables(positions[0])
        share = gain1.shape[0]
        first_lane = lax.rem(lax.axis_index("wg") * share, LANES)
        stacked = jnp.stack([gain1, bias1, gain2, bias2])
        ln_part = lax.dynamic_update_slice(jnp.zeros((8, 4 * LANES), F32), stacked, (0, first_lane))
        y_out, k_heads, v_heads = run_layer(n, x_loc[0], lengths, cos_tab, sin_tab, ln_part, wq, wk, wv, wo, wu, wd, scale)
        return y_out[None], jnp.swapaxes(k_heads, 0, 1)[None], jnp.swapaxes(v_heads, 0, 1)[None]

    return jax.shard_map(local_layer, mesh=mesh, in_specs=(batch_spec, batch_spec, batch_spec) + (row_spec,) * 10,
                         out_specs=(batch_spec, batch_spec, batch_spec), check_vma=False)
```

```python
import functools
import math

import jax
import jax.numpy as jnp
from jax import lax
from jax.experimental import pallas as pl
from jax.experimental.pallas import tpu as pltpu
from jax.sharding import PartitionSpec as P

LN_EPS = 1e-5
ROPE_BASE = 10000.0
HEAD_DIM = 128
LANES = 128
MESH = pl.DeviceIdType.MESH
F32 = jnp.float32
BF16 = jnp.bfloat16


def rotary_tables(positions):
    quarter = HEAD_DIM // 4
    inv_freq = ROPE_BASE ** (-jnp.arange(quarter, dtype=F32) / quarter)
    angles = positions.astype(F32)[None, :] * inv_freq[:, None]
    return jnp.cos(angles), jnp.sin(angles)


def layer_kernel(cfg, len_ref, cos_ref, sin_ref, x_ref, ln_ref, wq_ref, wk_ref, wv_ref, wo_ref, wu_ref, wd_ref,
                 y_ref, k_out, v_out, gln, gq, gk, gv, go, gu, gd,
                 x_s, h_s, q_s, k_s, v_s, a_s, wb, wbd, acc_s, cos_s, sin_s, turn_s, lnv, lnbuf, lnst,
                 send_sem, recv_sem, stage_sem, own_sem, wb_sem, wbd_sem, io_sem):
    side = cfg["side"]
    seq, d_model = x_s.shape
    n_heads, n_kv = q_s.shape[0], k_s.shape[0]
    tile, rows_m = cfg["tile"], cfg["rows_m"]
    me = lax.axis_index("wg")
    c = lax.rem(me, 2)
    x = lax.rem(me // 2, side)
    y = me // (2 * side)
    xp, xm = lax.rem(x + 1, side), lax.rem(x + side - 1, side)
    yp, ym = lax.rem(y + 1, side), lax.rem(y + side - 1, side)
    xo, yo = lax.rem(x + 2, side), lax.rem(y + 2, side)

    def device(yy, xx, cc):
        return (yy * side + xx) * 2 + cc

    d_xp, d_xm, d_yp, d_ym = device(y, xp, c), device(y, xm, c), device(yp, x, c), device(ym, x, c)
    d_peer = device(y, x, 1 - c)

    barrier = pltpu.get_barrier_semaphore()
    for dev in (d_xp, d_xm, d_yp, d_ym, d_peer):
        pl.semaphore_signal(barrier, inc=1, device_id={"wg": dev}, device_id_type=MESH)
    pl.semaphore_wait(barrier, 5)

    shards = {"ln": (ln_ref, gln), "q": (wq_ref, gq), "k": (wk_ref, gk), "v": (wv_ref, gv), "o": (wo_ref, go),
              "u": (wu_ref, gu), "d": (wd_ref, gd)}
    blocks = cfg["blocks"]

    def put(blk, phase, src, dst, dev):
        pltpu.make_async_remote_copy(
            src_ref=src, dst_ref=dst, send_sem=send_sem.at[blk, phase], recv_sem=recv_sem.at[blk, phase],
            device_id={"wg": dev}, device_id_type=MESH).start()

    def same(blk, phase, ref, dev):
        put(blk, phase, ref, ref, dev)

    def cols_of(blk):
        name, c0, width = blocks[blk]
        half = width // 2
        return pl.ds(c0, half), pl.ds(c0 + half, half), pl.ds(c0, width)

    def parts_of(blk):
        name, c0, width = blocks[blk]
        half, quarter, depth = width // 2, width // 4, shards[name][0].shape[0]
        if quarter < cfg["lanes"]:
            rows = (pl.ds(0, depth // 2), pl.ds(depth // 2, depth // 2))
            return [(r, pl.ds(start, half)) for start in (c0, c0 + half) for r in rows]
        every = pl.ds(0, depth)
        return [(every, pl.ds(c0 + i * quarter, quarter)) for i in range(4)]

    def unit_refs(blk):
        name, c0, width = blocks[blk]
        g = shards[name][1]
        cw = pl.ds(c0, width)
        return (g.at[0, pl.ds(0, 2), 0, :, cw], g.at[0, 0, 0, :, cw], g.at[0, :, :, :, cw],
                g.at[0, :, 0, :, cw], g.at[:, :, 0, :, cw])

    def wait_on(ref, sem):
        pltpu.make_async_copy(ref, ref, sem).wait()

    def wait_recv(blk, phase):
        wait_on(unit_refs(blk)[phase], recv_sem.at[blk, phase])

    def wait_send(blk):
        for phase, ref in enumerate(unit_refs(blk)):
            wait_on(ref, send_sem.at[blk, phase])

    def phase_1a(blk):
        w, g = shards[blocks[blk][0]]
        ca, cb, cw = cols_of(blk)
        put(blk, 0, w.at[:, ca], g.at[y, x, c, :, ca], d_xp)
        put(blk, 0, w.at[:, ca], g.at[y, x, c, :, ca], d_xm)
        put(blk, 0, w.at[:, cb], g.at[y, x, c, :, cb], d_yp)
        put(blk, 0, w.at[:, cb], g.at[y, x, c, :, cb], d_ym)
        put(blk, 4, w.at[:, cw], g.at[y, x, c, :, cw], d_peer)

    def phase_1b(blk):
        g = shards[blocks[blk][0]][1]
        ca, cb, _ = cols_of(blk)
        a0, a1, b0, b1 = parts_of(blk)
        wait_recv(blk, 0)
        same(blk, 1, g.at[(y, xm, c) + a0], d_xp)
        same(blk, 1, g.at[(y, xp, c) + a1], d_xm)
        same(blk, 1, g.at[(ym, x, c) + b0], d_yp)
        same(blk, 1, g.at[(yp, x, c) + b1], d_ym)
        same(blk, 4, g.at[y, xm, c, :, ca], d_peer)
        same(blk, 4, g.at[y, xp, c, :, ca], d_peer)
        same(blk, 4, g.at[ym, x, c, :, cb], d_peer)
        same(blk, 4, g.at[yp, x, c, :, cb], d_peer)

    def phase_2a(blk):
        g = shards[blocks[blk][0]][1]
        ca, cb, _ = cols_of(blk)
        wait_recv(blk, 1)
        same(blk, 2, g.at[y, :, c, :, ca], d_yp)
        same(blk, 2, g.at[y, :, c, :, ca], d_ym)
        same(blk, 2, g.at[:, x, c, :, cb], d_xp)
        same(blk, 2, g.at[:, x, c, :, cb], d_xm)
        same(blk, 4, g.at[y, xo, c, :, ca], d_peer)
        same(blk, 4, g.at[yo, x, c, :, cb], d_peer)

    def phase_2b(blk):
        g = shards[blocks[blk][0]][1]
        ca, cb, _ = cols_of(blk)
        a0, a1, b0, b1 = parts_of(blk)
        every = pl.ds(0, side)
        same(blk, 3, g.at[(ym, every, c) + a0], d_yp)
        same(blk, 3, g.at[(yp, every, c) + a1], d_ym)
        same(blk, 3, g.at[(every, xm, c) + b0], d_xp)
        same(blk, 3, g.at[(every, xp, c) + b1], d_xm)
        same(blk, 4, g.at[ym, :, c, :, ca], d_peer)
        same(blk, 4, g.at[yp, :, c, :, ca], d_peer)
        same(blk, 4, g.at[:, xm, c, :, cb], d_peer)
        same(blk, 4, g.at[:, xp, c, :, cb], d_peer)

    def finish(blk):
        g = shards[blocks[blk][0]][1]
        ca, cb, _ = cols_of(blk)
        wait_recv(blk, 3)
        same(blk, 4, g.at[yo, :, c, :, ca], d_peer)
        same(blk, 4, g.at[:, xo, c, :, cb], d_peer)

    def ready(blk):
        wait_recv(blk, 4)

    n_blk = len(blocks)

    def service(j):
        wait_recv(j, 2)
        if j + 1 < n_blk - 1:
            phase_2a(j + 1)
        phase_2b(j)
        if j == n_blk - 3:
            phase_2a(n_blk - 1)
        if j + 3 < n_blk:
            phase_1b(j + 3)
        if j + 5 < n_blk:
            phase_1a(j + 5)

    def matmul_tiles(g, col0, n_tiles, epilogue):
        def fetch(t, slot):
            return pltpu.make_async_copy(
                g.at[:, :, :, :, pl.ds(pl.multiple_of(col0 + t * tile, LANES), tile)], wb.at[slot], wb_sem.at[slot])

        fetch(0, 0).start()

        @pl.loop(0, n_tiles)
        def _(t):
            slot = lax.rem(t, 2)

            @pl.when(t + 1 < n_tiles)
            def _():
                fetch(t + 1, lax.rem(t + 1, 2)).start()

            fetch(t, slot).wait()

            @pl.loop(0, seq // rows_m)
            def _(m):
                rows = pl.ds(pl.multiple_of(m * rows_m, rows_m), rows_m)
                weights = wb[slot].reshape(d_model, tile)
                epilogue(t, rows, m, jnp.dot(h_s[rows, :], weights, preferred_element_type=F32))

    lane = lax.broadcasted_iota(jnp.int32, (rows_m, HEAD_DIM), 1)
    eighth = HEAD_DIM // 4

    def rotate(vals, rows):
        swapped = jnp.where(lane < eighth, pltpu.roll(vals, HEAD_DIM - eighth, 1), pltpu.roll(vals, eighth, 1))
        turned = vals * cos_s[rows, :] + swapped * sin_s[rows, :]
        return jnp.where(lane < 2 * eighth, turned, vals)

    heads_per_tile = tile // HEAD_DIM
    length = len_ref[0]

    def q_tiles(col0, width):
        def epilogue(t, rows, m, acc):
            for i in range(heads_per_tile):
                part = acc[:, i * HEAD_DIM:(i + 1) * HEAD_DIM]
                q_s[col0 // HEAD_DIM + t * heads_per_tile + i, rows, :] = rotate(part, rows).astype(BF16)

        matmul_tiles(gq, col0, width // tile, epilogue)

    def kv_tiles(g, out, turn, width):
        def epilogue(t, rows, m, acc):
            token = m * rows_m + lax.broadcasted_iota(jnp.int32, (rows_m, HEAD_DIM), 0)
            for i in range(heads_per_tile):
                part = acc[:, i * HEAD_DIM:(i + 1) * HEAD_DIM]
                part = rotate(part, rows) if turn else part
                kept = jnp.where(token < length, part, 0.0).astype(BF16)
                out[t * heads_per_tile + i, rows, :] = kept

        matmul_tiles(g, 0, width // tile, epilogue)

    per_kv = n_heads // n_kv
    q_rows = cfg["q_rows"]
    score_scale = HEAD_DIM ** -0.5

    def attention(g_lo, g_hi):
        @pl.loop(g_lo, g_hi)
        def _(kv):
            for blk in range(seq // q_rows):
                lo, hi = blk * q_rows, (blk + 1) * q_rows
                key = lax.broadcasted_iota(jnp.int32, (q_rows, hi), 1)
                query = lo + lax.broadcasted_iota(jnp.int32, (q_rows, hi), 0)
                allowed = (key <= query) & (key < length)
                for i in range(per_kv):
                    head = kv * per_kv + i
                    scores = lax.dot_general(q_s[head, lo:hi, :], k_s[kv, :hi, :], (((1,), (1,)), ((), ())),
                                             preferred_element_type=F32) * score_scale
                    scores = jnp.where(allowed, scores, -1e30)
                    probs = jnp.exp(scores - jnp.max(scores, axis=1, keepdims=True))
                    probs = probs * (1.0 / jnp.sum(probs, axis=1, keepdims=True))
                    out = jnp.dot(probs.astype(BF16), v_s[kv, :hi, :], preferred_element_type=F32)
                    h_s[lo:hi, pl.ds(pl.multiple_of(head * HEAD_DIM, HEAD_DIM), HEAD_DIM)] = out.astype(BF16)

    def o_tiles(col0, width):
        def epilogue(t, rows, m, acc):
            cols = pl.ds(pl.multiple_of(col0 + t * tile, LANES), tile)
            x_s[rows, cols] = (x_s[rows, cols].astype(F32) + acc).astype(BF16)

        matmul_tiles(go, col0, width // tile, epilogue)

    def up_tiles(col0, width):
        def epilogue(t, rows, m, acc):
            cols = pl.ds(pl.multiple_of(col0 + t * tile, LANES), tile)
            a_s[rows, cols] = jnp.square(jnp.maximum(acc, 0.0)).astype(BF16)

        matmul_tiles(gu, col0, width // tile, epilogue)

    def down_pieces(first, count):
        width = tile // 2
        depth = a_s.shape[1] // side

        @pl.loop(0, count)
        def _(piece):
            cols = pl.ds(pl.multiple_of((first + piece) * width, LANES), width)

            def fetch(k, slot):
                return pltpu.make_async_copy(gd.at[k, :, :, :, cols], wbd.at[slot], wbd_sem.at[slot])

            fetch(0, 0).start()

            @pl.loop(0, side)
            def _(k):
                slot = lax.rem(k, 2)

                @pl.when(k + 1 < side)
                def _():
                    fetch(k + 1, lax.rem(k + 1, 2)).start()

                fetch(k, slot).wait()
                deep = pl.ds(pl.multiple_of(k * depth, LANES), depth)

                @pl.loop(0, seq // rows_m)
                def _(m):
                    rows = pl.ds(pl.multiple_of(m * rows_m, rows_m), rows_m)
                    part = jnp.dot(a_s[rows, deep], wbd[slot].reshape(depth, width), preferred_element_type=F32)
                    acc_s[rows, :] = jnp.where(k == 0, part, acc_s[rows, :] + part)

            @pl.loop(0, seq // rows_m)
            def _(m):
                rows = pl.ds(pl.multiple_of(m * rows_m, rows_m), rows_m)
                x_s[rows, cols] = (x_s[rows, cols].astype(F32) + acc_s[rows, :]).astype(BF16)

            pltpu.make_async_copy(x_s.at[:, cols], y_ref.at[:, cols], io_sem.at[3]).start()

    def make_tables():
        span = cfg["span"]

        @pl.loop(0, seq // span)
        def _(m):
            rows = pl.ds(pl.multiple_of(m * span, span), span)
            cos, sin = cos_ref[:, rows].T, sin_ref[:, rows].T
            pad = jnp.zeros((span, 2 * eighth), F32)
            cos_s[rows, :] = jnp.concatenate([cos, cos, pad], axis=1)
            sin_s[rows, :] = jnp.concatenate([-sin, sin, pad], axis=1)

    def heads_inward(src, out, sem):
        step = 64

        @pl.loop(0, seq // step)
        def _(m):
            rows = pl.ds(pl.multiple_of(m * step, step), step)
            turn_s[rows, :, :] = jnp.swapaxes(src[:, rows, :].astype(F32), 0, 1).astype(BF16)

        pltpu.make_async_copy(turn_s, out, sem).start()

    def gather_norms():
        pltpu.make_async_copy(gln.at[:, :, :, :, pl.ds(0, 2 * LANES)], lnbuf, io_sem.at[4]).start()
        wait_on(lnbuf, io_sem.at[4])
        lnv[...] = jnp.zeros_like(lnv)
        share = cfg["share"]
        for dev in range(2 * side * side):
            start = dev * share // LANES * LANES
            width = min(2 * LANES, d_model - start)
            lnv[:, start:start + width] += lnbuf[dev // (2 * side), dev // 2 % side, dev % 2, :, :width]

    ln_rows = cfg["ln_rows"]

    def normalize(which):
        @pl.loop(0, seq // ln_rows)
        def _(m):
            rows = pl.ds(pl.multiple_of(m * ln_rows, ln_rows), ln_rows)
            acts = x_s[rows, :].astype(F32)
            centered = acts - jnp.mean(acts, axis=1, keepdims=True)
            variance = jnp.mean(centered * centered, axis=1, keepdims=True)
            gain, bias = lnv[which:which + 1, :], lnv[which + 1:which + 2, :]
            h_s[rows, :] = (centered * lax.rsqrt(variance + LN_EPS) * (1.0 + gain) + bias).astype(BF16)

    for blk in range(3):
        phase_1a(blk)
    pltpu.make_async_copy(x_ref, x_s, io_sem.at[0]).start()
    staged = []
    for idx, (name, r0, c0) in enumerate(cfg["staging"]):
        src = shards[name][0]
        spot = a_s.at[pl.ds(r0, src.shape[0]), pl.ds(c0, src.shape[1])]
        staged.append((shards[name][1], spot, src))
        pltpu.make_async_copy(src, spot, stage_sem.at[idx]).start()
    staged.append((gln, lnst, ln_ref))
    pltpu.make_async_copy(ln_ref, lnst, stage_sem.at[len(staged) - 1]).start()
    for idx, (g, spot, src) in enumerate(staged):
        wait_on(spot, stage_sem.at[idx])
        pltpu.make_async_copy(spot, g.at[y, x, c], own_sem.at[idx]).start()
    phase_1b(0)
    phase_1a(3)
    for idx, (g, spot, src) in enumerate(staged):
        wait_on(spot, own_sem.at[idx])
    phase_2a(0)
    phase_1b(1)
    phase_1a(4)
    phase_1b(2)

    kv_width, q_half, up_part = gk.shape[-1], gq.shape[-1] // 2, gu.shape[-1] // 6

    def first_norm():
        wait_on(x_s, io_sem.at[0])
        gather_norms()
        normalize(0)

    def caches():
        heads_inward(k_s, k_out, io_sem.at[1])
        wait_on(turn_s, io_sem.at[1])
        heads_inward(v_s, v_out, io_sem.at[2])
        wait_on(turn_s, io_sem.at[2])

    half_kv = n_kv // 2

    def stage(j):
        service(j)
        if j == 2:
            ready(0)
            first_norm()
            make_tables()
        if j == 3:
            ready(1)
            kv_tiles(gk, k_s, True, kv_width)
        if j == 4:
            ready(2)
            kv_tiles(gv, v_s, False, kv_width)
        if j == 5:
            caches()
        if j == 6:
            ready(3)
            ready(4)
            q_tiles(0, 2 * q_half)
        if j == 7:
            attention(0, half_kv)
        if j == 8:
            attention(half_kv, n_kv)
        if j == 9:
            ready(5)
            ready(6)
            o_tiles(0, d_model)
        if j == 10:
            normalize(2)
            ready(7)
            ready(8)
            up_tiles(0, 2 * up_part)
        if j == 12:
            ready(9)
            ready(10)
            up_tiles(2 * up_part, 2 * up_part)
        if j == 14:
            ready(11)
            ready(12)
            up_tiles(4 * up_part, 2 * up_part)
        if j == 15:
            ready(13)
            down_pieces(0, 2)
        if j == 16:
            ready(14)
            down_pieces(2, 2)
        if j == 18:
            down_pieces(7, 1)
        if j == 19:
            down_pieces(9, 1)
        if j >= 1:
            finish(j - 1)
        if j == 16:
            ready(15)
            down_pieces(4, 2)
        if j == 17:
            ready(16)
            down_pieces(6, 1)
        if j == 18:
            ready(17)
            down_pieces(8, 1)
        if j == 19:
            finish(19)
            ready(18)
            down_pieces(10, 1)
            ready(19)
            down_pieces(11, 1)

    for j in range(n_blk):
        stage(j)
    wait_on(x_s, io_sem.at[3])
    for blk in range(n_blk):
        wait_send(blk)


def run_layer(n, x_loc, len_loc, cos_tab, sin_tab, ln_part, wq, wk, wv, wo, wu, wd, scale=1):
    seq, d_model = x_loc.shape
    side = math.isqrt(n // 2)
    tile = 512 // scale
    nq, nkv, ff = wq.shape[1], wk.shape[1], wu.shape[1]
    half = nq // 2
    blocks = [("ln", 0, ln_part.shape[1]), ("k", 0, nkv), ("v", 0, nkv), ("q", 0, half), ("q", half, half),
              ("o", 0, d_model // 2), ("o", d_model // 2, d_model // 2)]
    blocks += [("u", i * (ff // 6), ff // 6) for i in range(6)]
    blocks += [("d", i * tile, tile) for i in range(5)] + [("d", 5 * tile, tile // 2), ("d", 11 * tile // 2, tile // 2)]
    share = wq.shape[0]
    staging = [("q", 0, 0), ("k", 0, nq), ("v", 0, nq + nkv), ("o", 0, nq + 2 * nkv), ("u", share, 0), ("d", 2 * share, 0)]
    cfg = dict(side=side, tile=tile, rows_m=512 // scale, q_rows=256 // scale, ln_rows=64, share=share, blocks=blocks,
               staging=staging, lanes=LANES // scale, span=LANES)
    vmem, hbm = pltpu.VMEM, pl.BlockSpec(memory_space=pltpu.HBM)

    def gathered(part):
        return jax.ShapeDtypeStruct((side, side, 2) + part.shape, part.dtype)

    flops = 2 * seq * (d_model * (nq + 2 * nkv + ff) + nq * d_model + ff * d_model)
    outs = pl.pallas_call(
        functools.partial(layer_kernel, cfg),
        out_shape=[jax.ShapeDtypeStruct((seq, d_model), BF16), jax.ShapeDtypeStruct((seq, nkv // HEAD_DIM, HEAD_DIM), BF16),
                   jax.ShapeDtypeStruct((seq, nkv // HEAD_DIM, HEAD_DIM), BF16)]
        + [gathered(part) for part in (ln_part, wq, wk, wv, wo, wu, wd)],
        in_specs=[pl.BlockSpec(memory_space=pltpu.SMEM), pl.BlockSpec(memory_space=vmem), pl.BlockSpec(memory_space=vmem)] + [hbm] * 8,
        out_specs=[hbm] * 10,
        scratch_shapes=[
            vmem((seq, d_model), BF16), vmem((seq, d_model), BF16), vmem((nq // HEAD_DIM, seq, HEAD_DIM), BF16),
            vmem((nkv // HEAD_DIM, seq, HEAD_DIM), BF16), vmem((nkv // HEAD_DIM, seq, HEAD_DIM), BF16), vmem((seq, ff), BF16),
            vmem((2, side, side, 2, share, tile), BF16), vmem((2, side, 2, wd.shape[0], tile // 2), BF16), vmem((seq, tile // 2), F32),
            vmem((seq, HEAD_DIM), F32), vmem((seq, HEAD_DIM), F32), vmem((seq, nkv // HEAD_DIM, HEAD_DIM), BF16),
            vmem((ln_part.shape[0], d_model), F32), vmem((side, side, 2, ln_part.shape[0], 2 * LANES), F32), vmem(ln_part.shape, F32),
            pltpu.SemaphoreType.DMA((len(blocks), 5)), pltpu.SemaphoreType.DMA((len(blocks), 5)),
            pltpu.SemaphoreType.DMA((7,)), pltpu.SemaphoreType.DMA((7,)), pltpu.SemaphoreType.DMA((2,)),
            pltpu.SemaphoreType.DMA((2,)), pltpu.SemaphoreType.DMA((5,)),
        ],
        compiler_params=pltpu.CompilerParams(collective_id=0, has_side_effects=True, vmem_limit_bytes=67043328),
        cost_estimate=pl.CostEstimate(flops=flops, bytes_accessed=4 * n * wd.size, transcendentals=0),
    )(len_loc, cos_tab, sin_tab, x_loc, ln_part, wq, wk, wv, wo, wu, wd)
    return outs[:3]


def solution(mesh, scale=1):
    batch_spec = P(("rep", "wg"))
    row_spec = P("wg")
    n = mesh.shape["wg"]

    def local_layer(x_loc, lengths, positions, wq, wk, wv, wo, wu, wd, gain1, bias1, gain2, bias2):
        n_seq, seq, d_model = x_loc.shape
        cos_tab, sin_tab = rotary_tables(positions[0])
        share = gain1.shape[0]
        first_lane = lax.rem(lax.axis_index("wg") * share, LANES)
        stacked = jnp.stack([gain1, bias1, gain2, bias2])
        ln_part = lax.dynamic_update_slice(jnp.zeros((8, 4 * LANES), F32), stacked, (0, first_lane))
        y_out, k_cache, v_cache = run_layer(n, x_loc[0], lengths, cos_tab, sin_tab, ln_part, wq, wk, wv, wo, wu, wd, scale)
        return y_out[None], k_cache[None], v_cache[None]

    return jax.shard_map(local_layer, mesh=mesh, in_specs=(batch_spec, batch_spec, batch_spec) + (row_spec,) * 10,
                         out_specs=(batch_spec, batch_spec, batch_spec), check_vma=False)
```

```python
import functools
import math

import jax
import jax.numpy as jnp
from jax import lax
from jax.experimental import pallas as pl
from jax.experimental.pallas import tpu as pltpu
from jax.sharding import PartitionSpec as P

LN_EPS = 1e-5
ROPE_BASE = 10000.0
HEAD_DIM = 128
LANES = 128
MESH = pl.DeviceIdType.MESH
F32 = jnp.float32
BF16 = jnp.bfloat16


def rotary_tables(positions):
    quarter = HEAD_DIM // 4
    inv_freq = ROPE_BASE ** (-jnp.arange(quarter, dtype=F32) / quarter)
    angles = positions.astype(F32)[None, :] * inv_freq[:, None]
    return jnp.cos(angles), jnp.sin(angles)


def layer_kernel(cfg, len_ref, cos_ref, sin_ref, x_ref, ln_ref, wq_ref, wk_ref, wv_ref, wo_ref, wu_ref, wd_ref,
                 y_ref, k_out, v_out, gln, gq, gk, gv, go, gu, gd,
                 x_s, h_s, q_s, k_s, v_s, a_s, wb, wbd, acc_s, cos_s, sin_s, turn_s, lnv, lnbuf, lnst,
                 send_sem, recv_sem, stage_sem, own_sem, wb_sem, wbd_sem, io_sem):
    side = cfg["side"]
    seq, d_model = x_s.shape
    n_heads, n_kv = q_s.shape[0], k_s.shape[0]
    tile, rows_m = cfg["tile"], cfg["rows_m"]
    me = lax.axis_index("wg")
    c = lax.rem(me, 2)
    x = lax.rem(me // 2, side)
    y = me // (2 * side)
    xp, xm = lax.rem(x + 1, side), lax.rem(x + side - 1, side)
    yp, ym = lax.rem(y + 1, side), lax.rem(y + side - 1, side)
    xo, yo = lax.rem(x + 2, side), lax.rem(y + 2, side)

    def device(yy, xx, cc):
        return (yy * side + xx) * 2 + cc

    d_xp, d_xm, d_yp, d_ym = device(y, xp, c), device(y, xm, c), device(yp, x, c), device(ym, x, c)
    d_peer = device(y, x, 1 - c)

    barrier = pltpu.get_barrier_semaphore()
    for dev in (d_xp, d_xm, d_yp, d_ym, d_peer):
        pl.semaphore_signal(barrier, inc=1, device_id={"wg": dev}, device_id_type=MESH)
    pl.semaphore_wait(barrier, 5)

    shards = {"ln": (ln_ref, gln), "q": (wq_ref, gq), "k": (wk_ref, gk), "v": (wv_ref, gv), "o": (wo_ref, go),
              "u": (wu_ref, gu), "d": (wd_ref, gd)}
    blocks = cfg["blocks"]

    def put(blk, phase, src, dst, dev):
        pltpu.make_async_remote_copy(
            src_ref=src, dst_ref=dst, send_sem=send_sem.at[blk, phase], recv_sem=recv_sem.at[blk, phase],
            device_id={"wg": dev}, device_id_type=MESH).start()

    def same(blk, phase, ref, dev):
        put(blk, phase, ref, ref, dev)

    def cols_of(blk):
        name, c0, width = blocks[blk]
        half = width // 2
        return pl.ds(c0, half), pl.ds(c0 + half, half), pl.ds(c0, width)

    def parts_of(blk):
        name, c0, width = blocks[blk]
        half, quarter, depth = width // 2, width // 4, shards[name][0].shape[0]
        if quarter < cfg["lanes"]:
            rows = (pl.ds(0, depth // 2), pl.ds(depth // 2, depth // 2))
            return [(r, pl.ds(start, half)) for start in (c0, c0 + half) for r in rows]
        every = pl.ds(0, depth)
        return [(every, pl.ds(c0 + i * quarter, quarter)) for i in range(4)]

    def unit_refs(blk):
        name, c0, width = blocks[blk]
        g = shards[name][1]
        cw = pl.ds(c0, width)
        return (g.at[0, pl.ds(0, 2), 0, :, cw], g.at[0, 0, 0, :, cw], g.at[0, :, :, :, cw],
                g.at[0, :, 0, :, cw], g.at[:, :, 0, :, cw])

    def wait_on(ref, sem):
        pltpu.make_async_copy(ref, ref, sem).wait()

    def wait_recv(blk, phase):
        wait_on(unit_refs(blk)[phase], recv_sem.at[blk, phase])

    def wait_send(blk):
        for phase, ref in enumerate(unit_refs(blk)):
            wait_on(ref, send_sem.at[blk, phase])

    def phase_1a(blk):
        w, g = shards[blocks[blk][0]]
        ca, cb, cw = cols_of(blk)
        put(blk, 0, w.at[:, ca], g.at[y, x, c, :, ca], d_xp)
        put(blk, 0, w.at[:, ca], g.at[y, x, c, :, ca], d_xm)
        put(blk, 0, w.at[:, cb], g.at[y, x, c, :, cb], d_yp)
        put(blk, 0, w.at[:, cb], g.at[y, x, c, :, cb], d_ym)
        put(blk, 4, w.at[:, cw], g.at[y, x, c, :, cw], d_peer)

    def phase_1b(blk):
        g = shards[blocks[blk][0]][1]
        ca, cb, _ = cols_of(blk)
        a0, a1, b0, b1 = parts_of(blk)
        wait_recv(blk, 0)
        same(blk, 1, g.at[(y, xm, c) + a0], d_xp)
        same(blk, 1, g.at[(y, xp, c) + a1], d_xm)
        same(blk, 1, g.at[(ym, x, c) + b0], d_yp)
        same(blk, 1, g.at[(yp, x, c) + b1], d_ym)
        same(blk, 4, g.at[y, xm, c, :, ca], d_peer)
        same(blk, 4, g.at[y, xp, c, :, ca], d_peer)
        same(blk, 4, g.at[ym, x, c, :, cb], d_peer)
        same(blk, 4, g.at[yp, x, c, :, cb], d_peer)

    def phase_2a(blk):
        g = shards[blocks[blk][0]][1]
        ca, cb, _ = cols_of(blk)
        wait_recv(blk, 1)
        same(blk, 2, g.at[y, :, c, :, ca], d_yp)
        same(blk, 2, g.at[y, :, c, :, ca], d_ym)
        same(blk, 2, g.at[:, x, c, :, cb], d_xp)
        same(blk, 2, g.at[:, x, c, :, cb], d_xm)
        same(blk, 4, g.at[y, xo, c, :, ca], d_peer)
        same(blk, 4, g.at[yo, x, c, :, cb], d_peer)

    def phase_2b(blk):
        g = shards[blocks[blk][0]][1]
        ca, cb, _ = cols_of(blk)
        a0, a1, b0, b1 = parts_of(blk)
        every = pl.ds(0, side)
        same(blk, 3, g.at[(ym, every, c) + a0], d_yp)
        same(blk, 3, g.at[(yp, every, c) + a1], d_ym)
        same(blk, 3, g.at[(every, xm, c) + b0], d_xp)
        same(blk, 3, g.at[(every, xp, c) + b1], d_xm)
        same(blk, 4, g.at[ym, :, c, :, ca], d_peer)
        same(blk, 4, g.at[yp, :, c, :, ca], d_peer)
        same(blk, 4, g.at[:, xm, c, :, cb], d_peer)
        same(blk, 4, g.at[:, xp, c, :, cb], d_peer)

    def finish(blk):
        g = shards[blocks[blk][0]][1]
        ca, cb, _ = cols_of(blk)
        wait_recv(blk, 3)
        same(blk, 4, g.at[yo, :, c, :, ca], d_peer)
        same(blk, 4, g.at[:, xo, c, :, cb], d_peer)

    def ready(blk):
        wait_recv(blk, 4)

    n_blk = len(blocks)

    def service(j):
        wait_recv(j, 2)
        if j + 4 < n_blk:
            phase_1b(j + 4)
        if j + 6 < n_blk:
            phase_1a(j + 6)
        phase_2b(j)
        if j + 2 < n_blk:
            phase_2a(j + 2)

    def matmul_tiles(g, first, n_tiles, epilogue):
        def fetch(t, slot):
            return pltpu.make_async_copy(
                g.at[:, :, :, :, pl.ds(pl.multiple_of((first + t) * tile, LANES), tile)], wb.at[slot], wb_sem.at[slot])

        fetch(0, 0).start()

        @pl.loop(0, n_tiles)
        def _(t):
            slot = lax.rem(t, 2)

            @pl.when(t + 1 < n_tiles)
            def _():
                fetch(t + 1, lax.rem(t + 1, 2)).start()

            fetch(t, slot).wait()

            @pl.loop(0, seq // rows_m)
            def _(m):
                rows = pl.ds(pl.multiple_of(m * rows_m, rows_m), rows_m)
                weights = wb[slot].reshape(d_model, tile)
                epilogue(first + t, rows, m, jnp.dot(h_s[rows, :], weights, preferred_element_type=F32))

    lane = lax.broadcasted_iota(jnp.int32, (rows_m, HEAD_DIM), 1)
    eighth = HEAD_DIM // 4

    def rotate(vals, rows):
        swapped = jnp.where(lane < eighth, pltpu.roll(vals, HEAD_DIM - eighth, 1), pltpu.roll(vals, eighth, 1))
        turned = vals * cos_s[rows, :] + swapped * sin_s[rows, :]
        return jnp.where(lane < 2 * eighth, turned, vals)

    heads_per_tile = tile // HEAD_DIM
    length = len_ref[0]

    def q_tiles(first, count):
        def epilogue(t, rows, m, acc):
            for i in range(heads_per_tile):
                part = acc[:, i * HEAD_DIM:(i + 1) * HEAD_DIM]
                q_s[t * heads_per_tile + i, rows, :] = rotate(part, rows).astype(BF16)

        matmul_tiles(gq, first, count, epilogue)

    def kv_tiles(g, out, turn, width):
        def epilogue(t, rows, m, acc):
            token = m * rows_m + lax.broadcasted_iota(jnp.int32, (rows_m, HEAD_DIM), 0)
            for i in range(heads_per_tile):
                part = acc[:, i * HEAD_DIM:(i + 1) * HEAD_DIM]
                part = rotate(part, rows) if turn else part
                kept = jnp.where(token < length, part, 0.0).astype(BF16)
                out[t * heads_per_tile + i, rows, :] = kept

        matmul_tiles(g, 0, width // tile, epilogue)

    per_kv = n_heads // n_kv
    q_rows = cfg["q_rows"]
    score_scale = HEAD_DIM ** -0.5

    def attention(head_lo, head_hi):
        @pl.loop(head_lo, head_hi)
        def _(head):
            kv = head // per_kv
            for blk in range(seq // q_rows):
                lo, hi = blk * q_rows, (blk + 1) * q_rows
                key = lax.broadcasted_iota(jnp.int32, (q_rows, hi), 1)
                query = lo + lax.broadcasted_iota(jnp.int32, (q_rows, hi), 0)
                allowed = (key <= query) & (key < length)
                scores = lax.dot_general(q_s[head, lo:hi, :], k_s[kv, :hi, :], (((1,), (1,)), ((), ())),
                                         preferred_element_type=F32) * score_scale
                scores = jnp.where(allowed, scores, -1e30)
                probs = jnp.exp(scores - jnp.max(scores, axis=1, keepdims=True))
                probs = probs * (1.0 / jnp.sum(probs, axis=1, keepdims=True))
                out = jnp.dot(probs.astype(BF16), v_s[kv, :hi, :], preferred_element_type=F32)
                h_s[lo:hi, pl.ds(pl.multiple_of(head * HEAD_DIM, HEAD_DIM), HEAD_DIM)] = out.astype(BF16)

    def o_tiles(first, count):
        def epilogue(t, rows, m, acc):
            cols = pl.ds(pl.multiple_of(t * tile, LANES), tile)
            x_s[rows, cols] = (x_s[rows, cols].astype(F32) + acc).astype(BF16)

        matmul_tiles(go, first, count, epilogue)

    def up_tiles(first, count):
        def epilogue(t, rows, m, acc):
            cols = pl.ds(pl.multiple_of(t * tile, LANES), tile)
            a_s[rows, cols] = jnp.square(jnp.maximum(acc, 0.0)).astype(BF16)

        matmul_tiles(gu, first, count, epilogue)

    def down(col0, width, m_lo=0, m_hi=seq // rows_m):
        cols, wide = pl.ds(col0, width), pl.ds(0, width)
        depth = a_s.shape[1] // side

        def fetch(k, slot):
            return pltpu.make_async_copy(gd.at[k, :, :, :, cols], wbd.at[slot, :, :, :, wide], wbd_sem.at[slot])

        fetch(0, 0).start()

        @pl.loop(0, side)
        def _(k):
            slot = lax.rem(k, 2)

            @pl.when(k + 1 < side)
            def _():
                fetch(k + 1, lax.rem(k + 1, 2)).start()

            fetch(k, slot).wait()
            deep = pl.ds(pl.multiple_of(k * depth, LANES), depth)

            @pl.loop(m_lo, m_hi)
            def _(m):
                rows = pl.ds(pl.multiple_of(m * rows_m, rows_m), rows_m)
                weights = wbd[slot, :, :, :, wide].reshape(depth, width)
                part = jnp.dot(a_s[rows, deep], weights, preferred_element_type=F32)
                acc_s[rows, wide] = jnp.where(k == 0, part, acc_s[rows, wide] + part)

        @pl.loop(m_lo, m_hi)
        def _(m):
            rows = pl.ds(pl.multiple_of(m * rows_m, rows_m), rows_m)
            x_s[rows, cols] = (x_s[rows, cols].astype(F32) + acc_s[rows, wide]).astype(BF16)

        span = pl.ds(m_lo * rows_m, (m_hi - m_lo) * rows_m)
        pltpu.make_async_copy(x_s.at[span, cols], y_ref.at[span, cols], io_sem.at[3]).start()

    def make_tables():
        span = cfg["span"]

        @pl.loop(0, seq // span)
        def _(m):
            rows = pl.ds(pl.multiple_of(m * span, span), span)
            cos, sin = cos_ref[:, rows].T, sin_ref[:, rows].T
            pad = jnp.zeros((span, 2 * eighth), F32)
            cos_s[rows, :] = jnp.concatenate([cos, cos, pad], axis=1)
            sin_s[rows, :] = jnp.concatenate([-sin, sin, pad], axis=1)

    def heads_inward(src, out, sem):
        step = 64

        @pl.loop(0, seq // step)
        def _(m):
            rows = pl.ds(pl.multiple_of(m * step, step), step)
            turn_s[rows, :, :] = jnp.swapaxes(src[:, rows, :].astype(F32), 0, 1).astype(BF16)

        pltpu.make_async_copy(turn_s, out, sem).start()

    def gather_norms():
        pltpu.make_async_copy(gln.at[:, :, :, :, pl.ds(0, 2 * LANES)], lnbuf, io_sem.at[4]).start()
        wait_on(lnbuf, io_sem.at[4])
        lnv[...] = jnp.zeros_like(lnv)
        share = cfg["share"]
        for dev in range(2 * side * side):
            start = dev * share // LANES * LANES
            width = min(2 * LANES, d_model - start)
            lnv[:, start:start + width] += lnbuf[dev // (2 * side), dev // 2 % side, dev % 2, :, :width]

    ln_rows = cfg["ln_rows"]

    def normalize(which):
        @pl.loop(0, seq // ln_rows)
        def _(m):
            rows = pl.ds(pl.multiple_of(m * ln_rows, ln_rows), ln_rows)
            acts = x_s[rows, :].astype(F32)
            centered = acts - jnp.mean(acts, axis=1, keepdims=True)
            variance = jnp.mean(centered * centered, axis=1, keepdims=True)
            gain, bias = lnv[which:which + 1, :], lnv[which + 1:which + 2, :]
            h_s[rows, :] = (centered * lax.rsqrt(variance + LN_EPS) * (1.0 + gain) + bias).astype(BF16)

    for blk in range(3):
        phase_1a(blk)
    pltpu.make_async_copy(x_ref, x_s, io_sem.at[0]).start()
    staged = []
    for idx, (name, r0, c0) in enumerate(cfg["staging"]):
        src = shards[name][0]
        spot = a_s.at[pl.ds(r0, src.shape[0]), pl.ds(c0, src.shape[1])]
        staged.append((shards[name][1], spot, src))
        pltpu.make_async_copy(src, spot, stage_sem.at[idx]).start()
    staged.append((gln, lnst, ln_ref))
    pltpu.make_async_copy(ln_ref, lnst, stage_sem.at[len(staged) - 1]).start()
    for idx, (g, spot, src) in enumerate(staged):
        wait_on(spot, stage_sem.at[idx])
        pltpu.make_async_copy(spot, g.at[y, x, c], own_sem.at[idx]).start()
    phase_1b(0)
    phase_1a(3)
    phase_1a(4)
    for idx, (g, spot, src) in enumerate(staged):
        wait_on(spot, own_sem.at[idx])
    phase_2a(0)
    phase_1b(1)
    phase_1a(5)
    phase_1b(2)
    phase_2a(1)
    phase_1b(3)

    kv_width, halves = gk.shape[-1], seq // rows_m

    def first_norm():
        wait_on(x_s, io_sem.at[0])
        gather_norms()
        normalize(0)

    def caches():
        heads_inward(k_s, k_out, io_sem.at[1])
        wait_on(turn_s, io_sem.at[1])
        heads_inward(v_s, v_out, io_sem.at[2])
        wait_on(turn_s, io_sem.at[2])

    def arrive(*ids):
        for blk in ids:
            ready(blk)

    eighth_heads = n_heads // 8

    def stage(j):
        service(j)
        if j == 2:
            ready(0)
            first_norm()
            make_tables()
            finish(1)
            ready(1)
            kv_tiles(gk, k_s, True, kv_width)
        elif j == 3:
            finish(2)
            ready(2)
            kv_tiles(gv, v_s, False, kv_width)
        elif j == 4:
            finish(3)
            ready(3)
            q_tiles(0, 3)
        elif j == 5:
            caches()
            finish(4)
            ready(4)
            q_tiles(3, 3)
        elif j == 6:
            attention(0, 3 * eighth_heads)
            finish(5)
        elif j == 7:
            attention(3 * eighth_heads, 6 * eighth_heads)
            finish(6)
        elif j == 8:
            attention(6 * eighth_heads, n_heads)
            finish(7)
            arrive(5, 6)
            o_tiles(0, 2)
        elif j == 9:
            o_tiles(2, 4)
            finish(8)
            normalize(2)
        elif j == 10:
            arrive(7, 8)
            up_tiles(0, 5)
            finish(9)
        elif j == 11:
            arrive(9)
            up_tiles(5, 4)
            finish(10)
        elif j == 12:
            arrive(10)
            up_tiles(9, 3)
            finish(11)
        elif j == 13:
            arrive(11)
            up_tiles(12, 3)
            finish(12)
        elif j == 14:
            arrive(12)
            up_tiles(15, 3)
            finish(13)
        elif j == 15:
            arrive(13)
            down(0, tile)
            finish(14)
        elif j == 16:
            arrive(14)
            down(tile, tile)
            finish(15)
            ready(15)
            down(2 * tile, tile)
        elif j == 17:
            finish(16)
            ready(16)
            down(3 * tile, tile, 0, halves // 2)
        elif j == 18:
            down(3 * tile, tile, halves // 2, halves)
            finish(17)
            ready(17)
            down(4 * tile, tile, 0, halves // 2)
        elif j == 19:
            down(4 * tile, tile, halves // 2, halves)
            finish(18)
            finish(19)
            ready(18)
            down(5 * tile, tile // 2)
            ready(19)
            down(5 * tile + tile // 2, tile // 2)
        elif j == 1:
            finish(0)

    for j in range(n_blk):
        stage(j)
    wait_on(x_s, io_sem.at[3])
    for blk in range(n_blk):
        wait_send(blk)


def run_layer(n, x_loc, len_loc, cos_tab, sin_tab, ln_part, wq, wk, wv, wo, wu, wd, scale=1):
    seq, d_model = x_loc.shape
    side = math.isqrt(n // 2)
    tile = 512 // scale
    nq, nkv, ff = wq.shape[1], wk.shape[1], wu.shape[1]
    half = nq // 2
    blocks = [("ln", 0, ln_part.shape[1]), ("k", 0, nkv), ("v", 0, nkv), ("q", 0, half), ("q", half, half),
              ("o", 0, d_model // 2), ("o", d_model // 2, d_model // 2)]
    blocks += [("u", i * (ff // 6), ff // 6) for i in range(6)]
    blocks += [("d", i * tile, tile) for i in range(5)] + [("d", 5 * tile, tile // 2), ("d", 11 * tile // 2, tile // 2)]
    share = wq.shape[0]
    staging = [("q", 0, 0), ("k", 0, nq), ("v", 0, nq + nkv), ("o", 0, nq + 2 * nkv), ("u", share, 0), ("d", 2 * share, 0)]
    cfg = dict(side=side, tile=tile, rows_m=512 // scale, q_rows=256 // scale, ln_rows=64, share=share, blocks=blocks,
               staging=staging, lanes=LANES // scale, span=LANES)
    vmem, hbm = pltpu.VMEM, pl.BlockSpec(memory_space=pltpu.HBM)

    def gathered(part):
        return jax.ShapeDtypeStruct((side, side, 2) + part.shape, part.dtype)

    flops = 2 * seq * (d_model * (nq + 2 * nkv + ff) + nq * d_model + ff * d_model)
    outs = pl.pallas_call(
        functools.partial(layer_kernel, cfg),
        out_shape=[jax.ShapeDtypeStruct((seq, d_model), BF16), jax.ShapeDtypeStruct((seq, nkv // HEAD_DIM, HEAD_DIM), BF16),
                   jax.ShapeDtypeStruct((seq, nkv // HEAD_DIM, HEAD_DIM), BF16)]
        + [gathered(part) for part in (ln_part, wq, wk, wv, wo, wu, wd)],
        in_specs=[pl.BlockSpec(memory_space=pltpu.SMEM), pl.BlockSpec(memory_space=vmem), pl.BlockSpec(memory_space=vmem)] + [hbm] * 8,
        out_specs=[hbm] * 10,
        scratch_shapes=[
            vmem((seq, d_model), BF16), vmem((seq, d_model), BF16), vmem((nq // HEAD_DIM, seq, HEAD_DIM), BF16),
            vmem((nkv // HEAD_DIM, seq, HEAD_DIM), BF16), vmem((nkv // HEAD_DIM, seq, HEAD_DIM), BF16), vmem((seq, ff), BF16),
            vmem((2, side, side, 2, share, tile), BF16), vmem((2, side, 2, wd.shape[0], tile), BF16), vmem((seq, tile), F32),
            vmem((seq, HEAD_DIM), F32), vmem((seq, HEAD_DIM), F32), vmem((seq, nkv // HEAD_DIM, HEAD_DIM), BF16),
            vmem((ln_part.shape[0], d_model), F32), vmem((side, side, 2, ln_part.shape[0], 2 * LANES), F32), vmem(ln_part.shape, F32),
            pltpu.SemaphoreType.DMA((len(blocks), 5)), pltpu.SemaphoreType.DMA((len(blocks), 5)),
            pltpu.SemaphoreType.DMA((7,)), pltpu.SemaphoreType.DMA((7,)), pltpu.SemaphoreType.DMA((2,)),
            pltpu.SemaphoreType.DMA((2,)), pltpu.SemaphoreType.DMA((5,)),
        ],
        compiler_params=pltpu.CompilerParams(collective_id=0, has_side_effects=True, vmem_limit_bytes=67043328),
        cost_estimate=pl.CostEstimate(flops=flops, bytes_accessed=4 * n * wd.size, transcendentals=0),
    )(len_loc, cos_tab, sin_tab, x_loc, ln_part, wq, wk, wv, wo, wu, wd)
    return outs[:3]


def solution(mesh, scale=1):
    batch_spec = P(("rep", "wg"))
    row_spec = P("wg")
    n = mesh.shape["wg"]

    def local_layer(x_loc, lengths, positions, wq, wk, wv, wo, wu, wd, gain1, bias1, gain2, bias2):
        n_seq, seq, d_model = x_loc.shape
        cos_tab, sin_tab = rotary_tables(positions[0])
        share = gain1.shape[0]
        first_lane = lax.rem(lax.axis_index("wg") * share, LANES)
        stacked = jnp.stack([gain1, bias1, gain2, bias2])
        ln_part = lax.dynamic_update_slice(jnp.zeros((8, 4 * LANES), F32), stacked, (0, first_lane))
        y_out, k_cache, v_cache = run_layer(n, x_loc[0], lengths, cos_tab, sin_tab, ln_part, wq, wk, wv, wo, wu, wd, scale)
        return y_out[None], k_cache[None], v_cache[None]

    return jax.shard_map(local_layer, mesh=mesh, in_specs=(batch_spec, batch_spec, batch_spec) + (row_spec,) * 10,
                         out_specs=(batch_spec, batch_spec, batch_spec), check_vma=False)
```

```python
import functools
import math

import jax
import jax.numpy as jnp
from jax import lax
from jax.experimental import pallas as pl
from jax.experimental.pallas import tpu as pltpu
from jax.sharding import PartitionSpec as P

LN_EPS = 1e-5
ROPE_BASE = 10000.0
HEAD_DIM = 128
LANES = 128
MESH = pl.DeviceIdType.MESH
F32 = jnp.float32
BF16 = jnp.bfloat16


def rotary_tables(positions):
    quarter = HEAD_DIM // 4
    inv_freq = ROPE_BASE ** (-jnp.arange(quarter, dtype=F32) / quarter)
    angles = positions.astype(F32)[None, :] * inv_freq[:, None]
    return jnp.cos(angles), jnp.sin(angles)


def layer_kernel(cfg, len_ref, cos_ref, sin_ref, x_ref, ln_ref, wq_ref, wk_ref, wv_ref, wo_ref, wu_ref, wd_ref,
                 y_ref, k_out, v_out, gln, gq, gk, gv, go, gu, gd,
                 x_s, h_s, q_s, k_s, v_s, a_s, wb, wbd, acc_s, cos_s, sin_s, turn_s, lnv, lnbuf, lnst,
                 send_sem, recv_sem, stage_sem, own_sem, wb_sem, wbd_sem, io_sem):
    side = cfg["side"]
    seq, d_model = x_s.shape
    n_heads, n_kv = q_s.shape[0], k_s.shape[0]
    tile, rows_m = cfg["tile"], cfg["rows_m"]
    me = lax.axis_index("wg")
    c = lax.rem(me, 2)
    x = lax.rem(me // 2, side)
    y = me // (2 * side)
    xp, xm = lax.rem(x + 1, side), lax.rem(x + side - 1, side)
    yp, ym = lax.rem(y + 1, side), lax.rem(y + side - 1, side)
    xo, yo = lax.rem(x + 2, side), lax.rem(y + 2, side)

    def device(yy, xx, cc):
        return (yy * side + xx) * 2 + cc

    d_xp, d_xm, d_yp, d_ym = device(y, xp, c), device(y, xm, c), device(yp, x, c), device(ym, x, c)
    d_peer = device(y, x, 1 - c)

    barrier = pltpu.get_barrier_semaphore()
    for dev in (d_xp, d_xm, d_yp, d_ym, d_peer):
        pl.semaphore_signal(barrier, inc=1, device_id={"wg": dev}, device_id_type=MESH)
    pl.semaphore_wait(barrier, 5)

    shards = {"ln": (ln_ref, gln), "q": (wq_ref, gq), "k": (wk_ref, gk), "v": (wv_ref, gv), "o": (wo_ref, go),
              "u": (wu_ref, gu), "d": (wd_ref, gd)}
    blocks = cfg["blocks"]

    def put(blk, phase, src, dst, dev):
        pltpu.make_async_remote_copy(
            src_ref=src, dst_ref=dst, send_sem=send_sem.at[blk, phase], recv_sem=recv_sem.at[blk, phase],
            device_id={"wg": dev}, device_id_type=MESH).start()

    def same(blk, phase, ref, dev):
        put(blk, phase, ref, ref, dev)

    def cols_of(blk):
        name, c0, width = blocks[blk]
        half = width // 2
        return pl.ds(c0, half), pl.ds(c0 + half, half), pl.ds(c0, width)

    def parts_of(blk):
        name, c0, width = blocks[blk]
        half, quarter, depth = width // 2, width // 4, shards[name][0].shape[0]
        if quarter < cfg["lanes"]:
            rows = (pl.ds(0, depth // 2), pl.ds(depth // 2, depth // 2))
            return [(r, pl.ds(start, half)) for start in (c0, c0 + half) for r in rows]
        every = pl.ds(0, depth)
        return [(every, pl.ds(c0 + i * quarter, quarter)) for i in range(4)]

    def unit_refs(blk):
        name, c0, width = blocks[blk]
        g = shards[name][1]
        cw = pl.ds(c0, width)
        return (g.at[0, pl.ds(0, 2), 0, :, cw], g.at[0, 0, 0, :, cw], g.at[0, :, :, :, cw],
                g.at[0, :, 0, :, cw], g.at[:, :, 0, :, cw])

    def wait_on(ref, sem):
        pltpu.make_async_copy(ref, ref, sem).wait()

    def wait_recv(blk, phase):
        wait_on(unit_refs(blk)[phase], recv_sem.at[blk, phase])

    def wait_send(blk):
        for phase, ref in enumerate(unit_refs(blk)):
            wait_on(ref, send_sem.at[blk, phase])

    def phase_1a(blk):
        w, g = shards[blocks[blk][0]]
        ca, cb, cw = cols_of(blk)
        put(blk, 0, w.at[:, ca], g.at[y, x, c, :, ca], d_xp)
        put(blk, 0, w.at[:, ca], g.at[y, x, c, :, ca], d_xm)
        put(blk, 0, w.at[:, cb], g.at[y, x, c, :, cb], d_yp)
        put(blk, 0, w.at[:, cb], g.at[y, x, c, :, cb], d_ym)
        put(blk, 4, w.at[:, cw], g.at[y, x, c, :, cw], d_peer)

    def phase_1b(blk):
        g = shards[blocks[blk][0]][1]
        ca, cb, _ = cols_of(blk)
        a0, a1, b0, b1 = parts_of(blk)
        wait_recv(blk, 0)
        same(blk, 1, g.at[(y, xm, c) + a0], d_xp)
        same(blk, 1, g.at[(y, xp, c) + a1], d_xm)
        same(blk, 1, g.at[(ym, x, c) + b0], d_yp)
        same(blk, 1, g.at[(yp, x, c) + b1], d_ym)
        same(blk, 4, g.at[y, xm, c, :, ca], d_peer)
        same(blk, 4, g.at[y, xp, c, :, ca], d_peer)
        same(blk, 4, g.at[ym, x, c, :, cb], d_peer)
        same(blk, 4, g.at[yp, x, c, :, cb], d_peer)

    def phase_2a(blk):
        g = shards[blocks[blk][0]][1]
        ca, cb, _ = cols_of(blk)
        wait_recv(blk, 1)
        same(blk, 2, g.at[y, :, c, :, ca], d_yp)
        same(blk, 2, g.at[y, :, c, :, ca], d_ym)
        same(blk, 2, g.at[:, x, c, :, cb], d_xp)
        same(blk, 2, g.at[:, x, c, :, cb], d_xm)
        same(blk, 4, g.at[y, xo, c, :, ca], d_peer)
        same(blk, 4, g.at[yo, x, c, :, cb], d_peer)

    def phase_2b(blk):
        g = shards[blocks[blk][0]][1]
        ca, cb, _ = cols_of(blk)
        a0, a1, b0, b1 = parts_of(blk)
        every = pl.ds(0, side)
        same(blk, 3, g.at[(ym, every, c) + a0], d_yp)
        same(blk, 3, g.at[(yp, every, c) + a1], d_ym)
        same(blk, 3, g.at[(every, xm, c) + b0], d_xp)
        same(blk, 3, g.at[(every, xp, c) + b1], d_xm)
        same(blk, 4, g.at[ym, :, c, :, ca], d_peer)
        same(blk, 4, g.at[yp, :, c, :, ca], d_peer)
        same(blk, 4, g.at[:, xm, c, :, cb], d_peer)
        same(blk, 4, g.at[:, xp, c, :, cb], d_peer)

    def finish(blk):
        g = shards[blocks[blk][0]][1]
        ca, cb, _ = cols_of(blk)
        wait_recv(blk, 3)
        same(blk, 4, g.at[yo, :, c, :, ca], d_peer)
        same(blk, 4, g.at[:, xo, c, :, cb], d_peer)

    def ready(blk):
        wait_recv(blk, 4)

    n_blk = len(blocks)

    def service(j):
        wait_recv(j, 2)
        if j + 4 < n_blk:
            phase_1b(j + 4)
        if j + 6 < n_blk:
            phase_1a(j + 6)
        phase_2b(j)
        if j + 2 < n_blk:
            phase_2a(j + 2)

    def matmul_tiles(g, first, n_tiles, epilogue):
        def fetch(t, slot):
            return pltpu.make_async_copy(
                g.at[:, :, :, :, pl.ds(pl.multiple_of((first + t) * tile, LANES), tile)], wb.at[slot], wb_sem.at[slot])

        fetch(0, 0).start()

        @pl.loop(0, n_tiles)
        def _(t):
            slot = lax.rem(t, 2)

            @pl.when(t + 1 < n_tiles)
            def _():
                fetch(t + 1, lax.rem(t + 1, 2)).start()

            fetch(t, slot).wait()

            @pl.loop(0, seq // rows_m)
            def _(m):
                rows = pl.ds(pl.multiple_of(m * rows_m, rows_m), rows_m)
                weights = wb[slot].reshape(d_model, tile)
                epilogue(first + t, rows, m, jnp.dot(h_s[rows, :], weights, preferred_element_type=F32))

    lane = lax.broadcasted_iota(jnp.int32, (rows_m, HEAD_DIM), 1)
    eighth = HEAD_DIM // 4

    def rotate(vals, rows):
        swapped = jnp.where(lane < eighth, pltpu.roll(vals, HEAD_DIM - eighth, 1), pltpu.roll(vals, eighth, 1))
        turned = vals * cos_s[rows, :] + swapped * sin_s[rows, :]
        return jnp.where(lane < 2 * eighth, turned, vals)

    heads_per_tile = tile // HEAD_DIM
    length = len_ref[0]

    def q_tiles(first, count):
        def epilogue(t, rows, m, acc):
            for i in range(heads_per_tile):
                part = acc[:, i * HEAD_DIM:(i + 1) * HEAD_DIM]
                q_s[t * heads_per_tile + i, rows, :] = rotate(part, rows).astype(BF16)

        matmul_tiles(gq, first, count, epilogue)

    def kv_tiles(g, out, turn, width):
        def epilogue(t, rows, m, acc):
            token = m * rows_m + lax.broadcasted_iota(jnp.int32, (rows_m, HEAD_DIM), 0)
            for i in range(heads_per_tile):
                part = acc[:, i * HEAD_DIM:(i + 1) * HEAD_DIM]
                part = rotate(part, rows) if turn else part
                kept = jnp.where(token < length, part, 0.0).astype(BF16)
                out[t * heads_per_tile + i, rows, :] = kept

        matmul_tiles(g, 0, width // tile, epilogue)

    per_kv = n_heads // n_kv
    q_rows = cfg["q_rows"]
    score_scale = HEAD_DIM ** -0.5

    def attention(head_lo, head_hi):
        @pl.loop(head_lo, head_hi)
        def _(head):
            kv = head // per_kv
            for blk in range(seq // q_rows):
                lo, hi = blk * q_rows, (blk + 1) * q_rows
                key = lax.broadcasted_iota(jnp.int32, (q_rows, hi), 1)
                query = lo + lax.broadcasted_iota(jnp.int32, (q_rows, hi), 0)
                allowed = (key <= query) & (key < length)
                scores = lax.dot_general(q_s[head, lo:hi, :], k_s[kv, :hi, :], (((1,), (1,)), ((), ())),
                                         preferred_element_type=F32) * score_scale
                scores = jnp.where(allowed, scores, -1e30)
                probs = jnp.exp(scores - jnp.max(scores, axis=1, keepdims=True))
                probs = probs * (1.0 / jnp.sum(probs, axis=1, keepdims=True))
                out = jnp.dot(probs.astype(BF16), v_s[kv, :hi, :], preferred_element_type=F32)
                h_s[lo:hi, pl.ds(pl.multiple_of(head * HEAD_DIM, HEAD_DIM), HEAD_DIM)] = out.astype(BF16)

    def o_tiles(first, count):
        def epilogue(t, rows, m, acc):
            cols = pl.ds(pl.multiple_of(t * tile, LANES), tile)
            x_s[rows, cols] = (x_s[rows, cols].astype(F32) + acc).astype(BF16)

        matmul_tiles(go, first, count, epilogue)

    def up_tiles(first, count):
        def epilogue(t, rows, m, acc):
            cols = pl.ds(pl.multiple_of(t * tile, LANES), tile)
            a_s[rows, cols] = jnp.square(jnp.maximum(acc, 0.0)).astype(BF16)

        matmul_tiles(gu, first, count, epilogue)

    def down(col0, width, m_lo=0, m_hi=seq // rows_m, primed=False, prime=False):
        cols, wide = pl.ds(col0, width), pl.ds(0, width)
        depth = a_s.shape[1] // side

        def fetch(k, slot):
            return pltpu.make_async_copy(gd.at[k, :, :, :, cols], wbd.at[slot, :, :, :, wide], wbd_sem.at[slot])

        if not primed:
            fetch(0, 0).start()

        @pl.loop(0, side)
        def _(k):
            slot = lax.rem(k, 2)

            @pl.when(k + 1 < side)
            def _():
                fetch(k + 1, lax.rem(k + 1, 2)).start()

            if prime:
                @pl.when(k + 1 == side)
                def _():
                    fetch(0, 0).start()

            fetch(k, slot).wait()
            deep = pl.ds(pl.multiple_of(k * depth, LANES), depth)

            @pl.loop(m_lo, m_hi)
            def _(m):
                rows = pl.ds(pl.multiple_of(m * rows_m, rows_m), rows_m)
                weights = wbd[slot, :, :, :, wide].reshape(depth, width)
                part = jnp.dot(a_s[rows, deep], weights, preferred_element_type=F32)
                acc_s[rows, wide] = jnp.where(k == 0, part, acc_s[rows, wide] + part)

        @pl.loop(m_lo, m_hi)
        def _(m):
            rows = pl.ds(pl.multiple_of(m * rows_m, rows_m), rows_m)
            x_s[rows, cols] = (x_s[rows, cols].astype(F32) + acc_s[rows, wide]).astype(BF16)

        span = pl.ds(m_lo * rows_m, (m_hi - m_lo) * rows_m)
        pltpu.make_async_copy(x_s.at[span, cols], y_ref.at[span, cols], io_sem.at[3]).start()

    def make_tables():
        span = cfg["span"]

        @pl.loop(0, seq // span)
        def _(m):
            rows = pl.ds(pl.multiple_of(m * span, span), span)
            cos, sin = cos_ref[:, rows].T, sin_ref[:, rows].T
            pad = jnp.zeros((span, 2 * eighth), F32)
            cos_s[rows, :] = jnp.concatenate([cos, cos, pad], axis=1)
            sin_s[rows, :] = jnp.concatenate([-sin, sin, pad], axis=1)

    def heads_inward(src, out, sem):
        step = 64

        @pl.loop(0, seq // step)
        def _(m):
            rows = pl.ds(pl.multiple_of(m * step, step), step)
            turn_s[rows, :, :] = jnp.swapaxes(src[:, rows, :].astype(F32), 0, 1).astype(BF16)

        pltpu.make_async_copy(turn_s, out, sem).start()

    def gather_norms():
        pltpu.make_async_copy(gln.at[:, :, :, :, pl.ds(0, 2 * LANES)], lnbuf, io_sem.at[4]).start()
        wait_on(lnbuf, io_sem.at[4])
        lnv[...] = jnp.zeros_like(lnv)
        share = cfg["share"]
        for dev in range(2 * side * side):
            start = dev * share // LANES * LANES
            width = min(2 * LANES, d_model - start)
            lnv[:, start:start + width] += lnbuf[dev // (2 * side), dev // 2 % side, dev % 2, :, :width]

    ln_rows = cfg["ln_rows"]

    def normalize(which):
        @pl.loop(0, seq // ln_rows)
        def _(m):
            rows = pl.ds(pl.multiple_of(m * ln_rows, ln_rows), ln_rows)
            acts = x_s[rows, :].astype(F32)
            centered = acts - jnp.mean(acts, axis=1, keepdims=True)
            variance = jnp.mean(centered * centered, axis=1, keepdims=True)
            gain, bias = lnv[which:which + 1, :], lnv[which + 1:which + 2, :]
            h_s[rows, :] = (centered * lax.rsqrt(variance + LN_EPS) * (1.0 + gain) + bias).astype(BF16)

    for blk in range(3):
        phase_1a(blk)
    pltpu.make_async_copy(x_ref, x_s, io_sem.at[0]).start()
    staged = []
    for idx, (name, r0, c0) in enumerate(cfg["staging"]):
        src = shards[name][0]
        spot = a_s.at[pl.ds(r0, src.shape[0]), pl.ds(c0, src.shape[1])]
        staged.append((shards[name][1], spot, src))
        pltpu.make_async_copy(src, spot, stage_sem.at[idx]).start()
    staged.append((gln, lnst, ln_ref))
    pltpu.make_async_copy(ln_ref, lnst, stage_sem.at[len(staged) - 1]).start()
    for idx, (g, spot, src) in enumerate(staged):
        wait_on(spot, stage_sem.at[idx])
        pltpu.make_async_copy(spot, g.at[y, x, c], own_sem.at[idx]).start()
    phase_1b(0)
    phase_1a(3)
    phase_1a(4)
    for idx, (g, spot, src) in enumerate(staged):
        wait_on(spot, own_sem.at[idx])
    phase_2a(0)
    phase_1b(1)
    phase_1a(5)
    phase_1b(2)
    phase_2a(1)
    phase_1b(3)

    kv_width, halves = gk.shape[-1], seq // rows_m

    def first_norm():
        wait_on(x_s, io_sem.at[0])
        gather_norms()
        normalize(0)

    def caches():
        heads_inward(k_s, k_out, io_sem.at[1])
        wait_on(turn_s, io_sem.at[1])
        heads_inward(v_s, v_out, io_sem.at[2])
        wait_on(turn_s, io_sem.at[2])

    def arrive(*ids):
        for blk in ids:
            ready(blk)

    eighth_heads = n_heads // 8

    def stage(j):
        service(j)
        if j == 2:
            ready(0)
            first_norm()
            make_tables()
            finish(1)
            ready(1)
            kv_tiles(gk, k_s, True, kv_width)
        elif j == 3:
            finish(2)
            ready(2)
            kv_tiles(gv, v_s, False, kv_width)
        elif j == 4:
            finish(3)
            ready(3)
            q_tiles(0, 3)
        elif j == 5:
            caches()
            finish(4)
            ready(4)
            q_tiles(3, 3)
        elif j == 6:
            attention(0, 3 * eighth_heads)
            finish(5)
        elif j == 7:
            attention(3 * eighth_heads, 6 * eighth_heads)
            finish(6)
        elif j == 8:
            attention(6 * eighth_heads, n_heads)
            finish(7)
            arrive(5, 6)
            o_tiles(0, 2)
        elif j == 9:
            o_tiles(2, 4)
            finish(8)
            normalize(2)
        elif j == 10:
            arrive(7, 8)
            up_tiles(0, 5)
            finish(9)
        elif j == 11:
            arrive(9)
            up_tiles(5, 4)
            finish(10)
        elif j == 12:
            arrive(10)
            up_tiles(9, 3)
            finish(11)
        elif j == 13:
            arrive(11)
            up_tiles(12, 3)
            finish(12)
        elif j == 14:
            arrive(12)
            up_tiles(15, 3)
            finish(13)
        elif j == 15:
            arrive(13)
            down(0, tile)
            finish(14)
        elif j == 16:
            arrive(14)
            down(tile, tile)
            finish(15)
            ready(15)
            down(2 * tile, tile)
        elif j == 17:
            finish(16)
            ready(16)
            down(3 * tile, tile, 0, halves // 2, prime=True)
        elif j == 18:
            down(3 * tile, tile, halves // 2, halves, primed=True)
            finish(17)
        elif j == 19:
            ready(17)
            down(4 * tile, tile, 0, halves // 2, prime=True)
            finish(18)
            finish(19)
            down(4 * tile, tile, halves // 2, halves, primed=True)
            arrive(18, 19)
            down(5 * tile, tile)
        elif j == 1:
            finish(0)

    for j in range(n_blk):
        stage(j)
    wait_on(x_s, io_sem.at[3])
    for blk in range(n_blk):
        wait_send(blk)


def run_layer(n, x_loc, len_loc, cos_tab, sin_tab, ln_part, wq, wk, wv, wo, wu, wd, scale=1):
    seq, d_model = x_loc.shape
    side = math.isqrt(n // 2)
    tile = 512 // scale
    nq, nkv, ff = wq.shape[1], wk.shape[1], wu.shape[1]
    half = nq // 2
    blocks = [("ln", 0, ln_part.shape[1]), ("k", 0, nkv), ("v", 0, nkv), ("q", 0, half), ("q", half, half),
              ("o", 0, d_model // 2), ("o", d_model // 2, d_model // 2)]
    blocks += [("u", i * (ff // 6), ff // 6) for i in range(6)]
    blocks += [("d", i * tile, tile) for i in range(5)] + [("d", 5 * tile, tile // 2), ("d", 11 * tile // 2, tile // 2)]
    share = wq.shape[0]
    staging = [("q", 0, 0), ("k", 0, nq), ("v", 0, nq + nkv), ("o", 0, nq + 2 * nkv), ("u", share, 0), ("d", 2 * share, 0)]
    cfg = dict(side=side, tile=tile, rows_m=512 // scale, q_rows=256 // scale, ln_rows=64, share=share, blocks=blocks,
               staging=staging, lanes=LANES // scale, span=LANES)
    vmem, hbm = pltpu.VMEM, pl.BlockSpec(memory_space=pltpu.HBM)

    def gathered(part):
        return jax.ShapeDtypeStruct((side, side, 2) + part.shape, part.dtype)

    flops = 2 * seq * (d_model * (nq + 2 * nkv + ff) + nq * d_model + ff * d_model)
    outs = pl.pallas_call(
        functools.partial(layer_kernel, cfg),
        out_shape=[jax.ShapeDtypeStruct((seq, d_model), BF16), jax.ShapeDtypeStruct((seq, nkv // HEAD_DIM, HEAD_DIM), BF16),
                   jax.ShapeDtypeStruct((seq, nkv // HEAD_DIM, HEAD_DIM), BF16)]
        + [gathered(part) for part in (ln_part, wq, wk, wv, wo, wu, wd)],
        in_specs=[pl.BlockSpec(memory_space=pltpu.SMEM), pl.BlockSpec(memory_space=vmem), pl.BlockSpec(memory_space=vmem)] + [hbm] * 8,
        out_specs=[hbm] * 10,
        scratch_shapes=[
            vmem((seq, d_model), BF16), vmem((seq, d_model), BF16), vmem((nq // HEAD_DIM, seq, HEAD_DIM), BF16),
            vmem((nkv // HEAD_DIM, seq, HEAD_DIM), BF16), vmem((nkv // HEAD_DIM, seq, HEAD_DIM), BF16), vmem((seq, ff), BF16),
            vmem((2, side, side, 2, share, tile), BF16), vmem((2, side, 2, wd.shape[0], tile), BF16), vmem((seq, tile), F32),
            vmem((seq, HEAD_DIM), F32), vmem((seq, HEAD_DIM), F32), vmem((seq, nkv // HEAD_DIM, HEAD_DIM), BF16),
            vmem((ln_part.shape[0], d_model), F32), vmem((side, side, 2, ln_part.shape[0], 2 * LANES), F32), vmem(ln_part.shape, F32),
            pltpu.SemaphoreType.DMA((len(blocks), 5)), pltpu.SemaphoreType.DMA((len(blocks), 5)),
            pltpu.SemaphoreType.DMA((7,)), pltpu.SemaphoreType.DMA((7,)), pltpu.SemaphoreType.DMA((2,)),
            pltpu.SemaphoreType.DMA((2,)), pltpu.SemaphoreType.DMA((5,)),
        ],
        compiler_params=pltpu.CompilerParams(collective_id=0, has_side_effects=True, vmem_limit_bytes=67043328),
        cost_estimate=pl.CostEstimate(flops=flops, bytes_accessed=4 * n * wd.size, transcendentals=0),
    )(len_loc, cos_tab, sin_tab, x_loc, ln_part, wq, wk, wv, wo, wu, wd)
    return outs[:3]


def solution(mesh, scale=1):
    batch_spec = P(("rep", "wg"))
    row_spec = P("wg")
    n = mesh.shape["wg"]

    def local_layer(x_loc, lengths, positions, wq, wk, wv, wo, wu, wd, gain1, bias1, gain2, bias2):
        n_seq, seq, d_model = x_loc.shape
        cos_tab, sin_tab = rotary_tables(positions[0])
        share = gain1.shape[0]
        first_lane = lax.rem(lax.axis_index("wg") * share, LANES)
        stacked = jnp.stack([gain1, bias1, gain2, bias2])
        ln_part = lax.dynamic_update_slice(jnp.zeros((8, 4 * LANES), F32), stacked, (0, first_lane))
        y_out, k_cache, v_cache = run_layer(n, x_loc[0], lengths, cos_tab, sin_tab, ln_part, wq, wk, wv, wo, wu, wd, scale)
        return y_out[None], k_cache[None], v_cache[None]

    return jax.shard_map(local_layer, mesh=mesh, in_specs=(batch_spec, batch_spec, batch_spec) + (row_spec,) * 10,
                         out_specs=(batch_spec, batch_spec, batch_spec), check_vma=False)
```
